512 devices in a mesh: wide: 32 (over z_lo, y), narrow: 16 (over z_hi, x, core).
Axes of the slice: x: 4, y: 8, z: 8 (z_hi: 2, z_lo: 4; z = z_hi * 4 + z_lo), core: 2. Of those that a mesh axis runs over, the one named last changes fastest.
Arguments:
- stored_features: bfloat16 [64, 64, 64, 128], P(None, 'wide', 'narrow'), may hold values from -127 to 127
- channel_scale: float32 [64], replicated, may hold values from 0.005 to 0.05
- channel_shift: float32 [64], replicated, may hold values from -0.5 to 0.5
- first_weight: bfloat16 [64, 1728], replicated, may hold values from -0.21875 to 0.21875
- second_weight: bfloat16 [128, 1728], replicated, may hold values from -0.21875 to 0.21875
- third_weight: bfloat16 [256, 3456], P('narrow'), may hold values from -0.15625 to 0.15625
Outputs:
- coarse_features: bfloat16 [256, 32, 2048], P('narrow', 'wide')
The draws below stay inside these ranges and needn't reach their ends.
All inputs are finite; a program needn't handle non-finite values.
Results may differ from the reference program's by a relative error of at most 0.0057.
Values may be sent and summed in bfloat16 or wider, within the bound.
A program may use at most 64 MiB of HBM per device.

```python
import math
import jax
import jax.numpy as jnp
from jax import lax

C1 = 64
C2 = 128
C3 = 256
LEN_W = 128
ND = 64
NH = 64


def level_of(rng, dims, shards, least, largest):
    def one(dim, blocks):
        heights = jax.random.uniform(jax.random.fold_in(jax.random.fold_in(rng, 6), dim), (blocks,), jnp.float32, least / len(shards), largest / len(shards))
        return jnp.repeat(jnp.exp(heights), dims[dim] // blocks).reshape((-1,) + (1,) * (len(dims) - dim - 1))

    gain = one(*shards[0])
    for cut in shards[1:]:
        gain = gain * one(*cut)
    return gain


def normal_values(stream_key, extent, deviation, bound, split=(), kind=jnp.bfloat16):
    values = jax.random.normal(stream_key, extent, jnp.float32) * deviation
    if len(split) > 0:
        values = level_of(stream_key, extent, split, -0.22, 0.18) * values
    return jnp.clip(values, min=-bound, max=bound).astype(kind)


def setup_inputs(seed: int = 0) -> dict:
    keys = jax.random.split(jax.random.key(seed), 7)
    stored_features = normal_values(keys[0], (C1, ND, NH, LEN_W), 40.0, 127.0, ((1, 32), (2, 16)))
    channel_scale = jnp.clip(jnp.exp(jax.random.uniform(keys[1], (C1,), jnp.float32, math.log(0.005), math.log(0.05))), 0.005, 0.05)
    channel_shift = jnp.clip(jax.random.uniform(keys[2], (C1,), jnp.float32, -0.5, 0.5), -0.5, 0.5)
    first_weight = normal_values(keys[3], (C1, 27 * C1), (27 * C1 // 2) ** -0.5, 0.21875)
    second_weight = normal_values(keys[4], (C2, 27 * C1), (27 * C1 // 2) ** -0.5, 0.21875)
    third_weight = normal_values(keys[5], (C3, 27 * C2), (27 * C2 // 2) ** -0.5, 0.15625, ((0, 16),))
    return {"stored_features": stored_features, "channel_scale": channel_scale, "channel_shift": channel_shift, "first_weight": first_weight, "second_weight": second_weight, "third_weight": third_weight}


def convolve(features, weight):
    out_channels = weight.shape[0]
    in_channels = features.shape[0]
    kernel = weight.astype(jnp.float32).reshape(out_channels, 3, 3, 3, in_channels).transpose(0, 4, 1, 2, 3)
    result = lax.conv_general_dilated(features.astype(jnp.float32)[None], kernel, (1, 1, 1), ((1, 1), (1, 1), (1, 1)), dimension_numbers=("NCDHW", "OIDHW", "NCDHW"), precision=lax.Precision.HIGHEST)
    return result[0]


def reference(stored_features, channel_scale, channel_shift, first_weight, second_weight, third_weight):
    features = (stored_features.astype(jnp.float32) * channel_scale[:, None, None, None] + channel_shift[:, None, None, None]).astype(jnp.bfloat16)
    first_hidden = jnp.maximum(convolve(features, first_weight), 0.0).astype(jnp.bfloat16)
    second_hidden = jnp.maximum(convolve(first_hidden, second_weight), 0.0).astype(jnp.bfloat16)
    channels, depth_cells, height_cells, width_cells = second_hidden.shape
    pooled = second_hidden.reshape(channels, depth_cells // 2, 2, height_cells // 2, 2, width_cells // 2, 2).max(axis=(2, 4, 6))
    coarse = jnp.maximum(convolve(pooled, third_weight), 0.0).astype(jnp.bfloat16)
    return coarse.reshape(coarse.shape[0], coarse.shape[1], -1)
```

```python
import functools

import jax
import jax.numpy as jnp
from jax import lax
from jax.experimental import pallas as pl
from jax.experimental.pallas import tpu as pltpu
from jax.sharding import PartitionSpec as P

BF = jnp.bfloat16
F32 = jnp.float32
MESH = pl.DeviceIdType.MESH

H0, D0, G0, P0, WX0, WZ0, WF0, WC0, A0 = 0, 2, 4, 8, 16, 19, 20, 23, 31
NSEM = A0 + 16


def kernel(nw, nn, x_ref, sc_ref, sh_ref, w1_ref, w2_ref, w3_ref, out_ref,
           xf, fb, xs1, xs2, w1p, w2p, pb, xs3, w3g, ob, ssem, rsem):
    w = lax.axis_index("wide")
    n = lax.axis_index("narrow")
    half = nn // 2
    zh = n // half
    within = n % half
    mate = n + 1 - 2 * (n % 2)
    zmate = (n + half) % nn

    def xmate(k):
        return zh * half + (within + 2 * k) % half

    def side(i):
        return i - 1

    wok = [w > 0, None, w < nw - 1]
    nok = [n > 0, None, n < nn - 1]

    def ok(i, j):
        if i == 1:
            return nok[j]
        if j == 1:
            return wok[i]
        return jnp.logical_and(wok[i], nok[j])

    near = [(i, j) for i in range(3) for j in range(3) if (i, j) != (1, 1)]

    barrier = pltpu.get_barrier_semaphore()
    for k in range(1, nn):
        pl.semaphore_signal(barrier, inc=1, device_id=(w, (n + k) % nn), device_id_type=MESH)
    for i in (0, 2):
        for j in range(3):
            @pl.when(ok(i, j))
            def _():
                pl.semaphore_signal(
                    barrier, inc=1, device_id=(w + side(i), n + side(j)), device_id_type=MESH
                )

    one = jnp.int32(1)
    zero = jnp.int32(0)
    wcount = jnp.where(w > 0, one, zero) + jnp.where(w < nw - 1, one, zero)
    ncount = jnp.where(n > 0, one, zero) + jnp.where(n < nn - 1, one, zero)
    expected = (nn - 1) + wcount * (1 + ncount)

    @pl.when(n == 0)
    def _():
        fb[:, :, 0:256] = jnp.zeros((6, 64, 256), BF)
        pb[:, 0] = jnp.zeros((3, 128, 128), BF)

    @pl.when(n == nn - 1)
    def _():
        fb[:, :, 768:1024] = jnp.zeros((6, 64, 256), BF)
        pb[:, 2] = jnp.zeros((3, 128, 128), BF)

    @pl.when(w == 0)
    def _():
        fb[0:2] = jnp.zeros((2, 64, 1024), BF)
        pb[0] = jnp.zeros((3, 128, 128), BF)

    @pl.when(w == nw - 1)
    def _():
        fb[4:6] = jnp.zeros((2, 64, 1024), BF)
        pb[2] = jnp.zeros((3, 128, 128), BF)

    lane = lax.broadcasted_iota(jnp.int32, (1, 128), 1)

    def shifted(t, period):
        pos = lane % period
        before = jnp.where(pos > 0, pltpu.roll(t, 1, 1), 0.0)
        after = jnp.where(pos < period - 1, pltpu.roll(t, 127, 1), 0.0)
        return before.astype(BF), t.astype(BF), after.astype(BF)

    def stack1(d, h):
        t = fb[d, :, h * 128:(h + 1) * 128].astype(F32)
        for e, v in enumerate(shifted(t, 128)):
            xs1[d * 192 + e * 64:d * 192 + (e + 1) * 64, h * 128:(h + 1) * 128] = v

    eye = lax.broadcasted_iota(jnp.int32, (64, 64), 0) == lax.broadcasted_iota(jnp.int32, (64, 64), 1)

    def column(ref):
        return jnp.sum(jnp.where(eye, ref[...], 0.0), axis=1, keepdims=True)

    scale = column(sc_ref)
    shift = column(sh_ref)
    xf[...] = x_ref[...].astype(F32)
    for d in range(2):
        for h in range(4):
            t = xf[pl.ds(d * 4 + h, 64, stride=8), :]
            fb[2 + d, :, (2 + h) * 128:(3 + h) * 128] = (t * scale + shift).astype(BF)

    for a in range(3):
        for b in range(3):
            c0 = (a * 3 + b) * 192
            w1p[b * 64:(b + 1) * 64, a * 192:(a + 1) * 192] = w1_ref[:, c0:c0 + 192]
            w2p[b * 128:(b + 1) * 128, a * 192:(a + 1) * 192] = w2_ref[:, c0:c0 + 192]
    w3g[pl.ds(pl.multiple_of(n * 16, 16), 16), :] = w3_ref[...]

    pl.semaphore_wait(barrier, expected)

    def remote(src, dst, s, dev, r=None):
        return pltpu.make_async_remote_copy(
            src_ref=src, dst_ref=dst, send_sem=ssem.at[s], recv_sem=rsem.at[s if r is None else r],
            device_id=dev, device_id_type=MESH,
        )

    lo, hi = slice(256, 512), slice(512, 768)
    c_h = [
        remote(fb.at[2:4, :, lo], fb.at[2:4, :, 768:1024], H0, (w, n - 1)),
        remote(fb.at[2:4, :, hi], fb.at[2:4, :, 0:256], H0 + 1, (w, n + 1)),
    ]
    h_send = [nok[0], nok[2]]
    h_recv = [nok[2], nok[0]]
    own = slice(256, 768)
    c_d = [
        remote(fb.at[2:4, :, own], fb.at[4:6, :, own], D0, (w - 1, n)),
        remote(fb.at[2:4, :, own], fb.at[0:2, :, own], D0 + 1, (w + 1, n)),
    ]
    d_send = [wok[0], wok[2]]
    d_recv = [wok[2], wok[0]]
    edge = [slice(0, 256), slice(768, 1024)]
    c_g, g_send, g_recv = [], [], []
    for k, (dst, dev) in enumerate((((4, 6), w - 1), ((0, 2), w + 1))):
        for j in range(2):
            c_g.append(
                remote(fb.at[2:4, :, edge[j]], fb.at[dst[0]:dst[1], :, edge[j]], G0 + 2 * k + j, (dev, n))
            )
            g_send.append(jnp.logical_and(d_send[k], nok[2 * j]))
            g_recv.append(jnp.logical_and(d_recv[k], nok[2 * j]))

    def when(cond, f):
        pl.when(cond)(f)

    for k in range(2):
        when(h_send[k], c_h[k].start)
    for k in range(2):
        when(d_send[k], c_d[k].start)

    def shard(m):
        return w3g.at[pl.ds(pl.multiple_of(m * 16, 16), 16), :]

    c_wx = [remote(w3_ref, shard(n), WX0 + k - 1, (w, xmate(k))) for k in range(1, 4)]
    c_wz = remote(w3_ref, shard(n), WZ0, (w, zmate))
    c_wf = [remote(shard(zmate), shard(zmate), WF0 + k - 1, (w, xmate(k))) for k in range(1, 4)]
    order = [n, xmate(1), xmate(2), xmate(3)]
    order = order + [(m + half) % nn for m in order]
    c_wc = [
        remote(w3_ref if k == 0 else shard(m), shard(m), WC0 + k, (w, mate))
        for k, m in enumerate(order)
    ]
    c_wz.start()
    for c in c_wx:
        c.start()
    c_wc[0].start()

    for d in (2, 3):
        for h in range(2, 6):
            stack1(d, h)

    for k in range(2):
        when(h_recv[k], c_h[k].wait_recv)
    for k in range(4):
        when(g_send[k], c_g[k].start)
    for d in (2, 3):
        for h in (0, 1, 6, 7):
            stack1(d, h)
    for k in range(2):
        when(d_recv[k], c_d[k].wait_recv)
    for d in (0, 1, 4, 5):
        for h in range(2, 6):
            stack1(d, h)
    for k in range(4):
        when(g_recv[k], c_g[k].wait_recv)
    for d in (0, 1, 4, 5):
        for h in (0, 1, 6, 7):
            stack1(d, h)

    c_wz.wait_recv()
    for c in c_wf:
        c.start()
    for k in range(3):
        c_wx[k].wait_recv()
    for k in range(1, 5):
        c_wc[k].start()

    lane6 = lax.broadcasted_iota(jnp.int32, (1, 768), 1)
    inside = jnp.logical_and(
        jnp.logical_or(lane6 >= 128, n > 0), jnp.logical_or(lane6 < 640, n < nn - 1)
    )

    def first(d, carry):
        y = jnp.dot(
            w1p[...], xs1[pl.ds(pl.multiple_of(d * 192, 192), 576), :], preferred_element_type=F32
        )
        y = y[0:64, 0:768] + y[64:128, 128:896] + y[128:192, 256:1024]
        level = 2 * w + d - 1
        keep = jnp.logical_and(inside, jnp.logical_and(level >= 0, level < 2 * nw))
        y = jnp.where(keep, jnp.maximum(y, 0.0), 0.0)
        for h in range(6):
            for e, v in enumerate(shifted(y[:, h * 128:(h + 1) * 128], 128)):
                xs2[pl.ds(pl.multiple_of(d * 192 + e * 64, 64), 64), h * 128:(h + 1) * 128] = v
        return carry

    lax.fori_loop(0, 4, first, 0)

    def second(d):
        y = jnp.dot(w2p[...], xs2[d * 192:d * 192 + 576, :], preferred_element_type=F32)
        return y[0:128, 0:512] + y[128:256, 128:640] + y[256:384, 256:768]

    s = jnp.maximum(jnp.maximum(second(0), second(1)), 0.0)
    rows = []
    for r in range(2):
        t = jnp.maximum(s[:, r * 256:r * 256 + 128], s[:, r * 256 + 128:r * 256 + 256])
        rows.append(jnp.maximum(t, pltpu.roll(t, 127, 1)).astype(BF))
    k_i = lax.broadcasted_iota(jnp.int32, (128, 128), 0)
    j_i = lax.broadcasted_iota(jnp.int32, (128, 128), 1)
    pick0 = jnp.where(k_i == 2 * j_i, 1.0, 0.0).astype(BF)
    pick1 = jnp.where(k_i == 2 * (j_i - 64), 1.0, 0.0).astype(BF)
    pooled = jnp.dot(rows[0], pick0, preferred_element_type=F32) + jnp.dot(
        rows[1], pick1, preferred_element_type=F32
    )
    pb[1, 1] = pooled.astype(BF)

    c_p = []
    for k, (i, j) in enumerate(near):
        c_p.append(
            remote(pb.at[1, 1], pb.at[2 - i, 2 - j], P0 + k, (w + side(i), n + side(j)))
        )
        when(ok(i, j), c_p[k].start)

    for c in c_wf:
        c.wait_recv()
    for k in range(5, 8):
        c_wc[k].start()

    for k, (i, j) in enumerate(near):
        when(ok(2 - i, 2 - j), c_p[k].wait_recv)

    low = lane < 64

    def coarse_stack(a, carry):
        left = pb[a, 0].astype(F32)
        mid = pb[a, 1].astype(F32)
        right = pb[a, 2].astype(F32)
        tops = (
            pltpu.roll(jnp.where(low, mid, left), 64, 1),
            mid,
            pltpu.roll(jnp.where(low, right, mid), 64, 1),
        )
        for b, t in enumerate(tops):
            for e, v in enumerate(shifted(t, 64)):
                xs3[pl.ds(pl.multiple_of(a * 1152 + (b * 3 + e) * 128, 128), 128), :] = v
        return carry

    lax.fori_loop(0, 3, coarse_stack, 0)

    for c in c_wc:
        c.wait_recv()

    def coarse(g, carry):
        y = jnp.dot(
            w3g[pl.ds(pl.multiple_of(g * 128, 128), 128), :], xs3[...], preferred_element_type=F32
        )
        ob[pl.ds(pl.multiple_of(g * 128, 128), 128), :] = jnp.maximum(y, 0.0).astype(BF)
        return carry

    lax.fori_loop(0, 2, coarse, 0)

    def block(m):
        return out_ref.at[:, pl.ds(pl.multiple_of(m * 128, 128), 128)]

    def piece(m):
        return ob.at[pl.ds(pl.multiple_of(m * 16, 16), 16), :]

    c_a = []
    for k in range(1, nn):
        m = (n + k) % nn
        c = remote(piece(m), block(n), A0 + k, (w, m))
        c.start()
        c_a.append(c)
    out_ref[:, pl.ds(pl.multiple_of(n * 128, 128), 128)] = ob[
        pl.ds(pl.multiple_of(n * 16, 16), 16), :
    ]

    for k in range(1, nn):
        src = (n - k + nn) % nn
        remote(piece(n), block(src), A0 + k, (w, src)).wait_recv()

    for k in range(2):
        when(h_send[k], c_h[k].wait_send)
        when(d_send[k], c_d[k].wait_send)
    for k in range(4):
        when(g_send[k], c_g[k].wait_send)
    for k, (i, j) in enumerate(near):
        when(ok(i, j), c_p[k].wait_send)
    c_wz.wait_send()
    for c in c_wx + c_wf + c_wc + c_a:
        c.wait_send()


def solution(mesh):
    nw, nn = mesh.shape["wide"], mesh.shape["narrow"]

    def body(stored_features, channel_scale, channel_shift, first_weight, second_weight, third_weight):
        x = stored_features.reshape(512, 128)
        out = pl.pallas_call(
            functools.partial(kernel, nw, nn),
            out_shape=jax.ShapeDtypeStruct((16, nn * 128), BF),
            in_specs=[pl.BlockSpec(memory_space=pltpu.VMEM)] * 6,
            out_specs=pl.BlockSpec(memory_space=pltpu.VMEM),
            scratch_shapes=[
                pltpu.VMEM((512, 128), F32),
                pltpu.VMEM((6, 64, 1024), BF),
                pltpu.VMEM((6 * 192, 1024), BF),
                pltpu.VMEM((4 * 192, 768), BF),
                pltpu.VMEM((192, 576), BF),
                pltpu.VMEM((384, 576), BF),
                pltpu.VMEM((3, 3, 128, 128), BF),
                pltpu.VMEM((3456, 128), BF),
                pltpu.VMEM((nn * 16, 3456), BF),
                pltpu.VMEM((256, 128), BF),
                pltpu.SemaphoreType.DMA((NSEM,)),
                pltpu.SemaphoreType.DMA((NSEM,)),
            ],
            compiler_params=pltpu.CompilerParams(collective_id=0, has_side_effects=True),
        )(x, channel_scale.reshape(1, 64), channel_shift.reshape(1, 64), first_weight, second_weight, third_weight)
        return out.reshape(16, 1, nn * 128)

    in_specs = (P(None, "wide", "narrow", None), P(), P(), P(), P(), P("narrow", None))
    return jax.shard_map(
        body, mesh=mesh, in_specs=in_specs, out_specs=P("narrow", "wide", None), check_vma=False
    )
```

```python
import functools

import jax
import jax.numpy as jnp
from jax import lax
from jax.experimental import pallas as pl
from jax.experimental.pallas import tpu as pltpu
from jax.sharding import PartitionSpec as P

BF = jnp.bfloat16
F32 = jnp.float32
MESH = pl.DeviceIdType.MESH

H0, D0, G0, P0, WX0, WZ0, WF0, WC0, A0 = 0, 2, 4, 8, 16, 19, 20, 23, 31
NSEM = A0 + 16


def kernel(nw, nn, x_ref, sc_ref, sh_ref, w1_ref, w2_ref, w3_ref, out_ref,
           xf, fb, xs1, xs2, w1p, w2p, pb, xs3, w3g, ob, ssem, rsem, fsem):
    w = lax.axis_index("wide")
    n = lax.axis_index("narrow")
    half = nn // 2
    zh = n // half
    within = n % half
    mate = n + 1 - 2 * (n % 2)
    zmate = (n + half) % nn

    def xmate(k):
        return zh * half + (within + 2 * k) % half

    def side(i):
        return i - 1

    wok = [w > 0, None, w < nw - 1]
    nok = [n > 0, None, n < nn - 1]

    def ok(i, j):
        if i == 1:
            return nok[j]
        if j == 1:
            return wok[i]
        return jnp.logical_and(wok[i], nok[j])

    near = [(i, j) for i in range(3) for j in range(3) if (i, j) != (1, 1)]

    early = zh == 0
    late = zh == 1
    flip = (nw // 8 - 1 - w // 8) * 8 + w % 8 if nw % 8 == 0 else w
    cross = [jnp.logical_and(n == half, late), None, jnp.logical_and(n == half - 1, early)]
    same = [jnp.logical_and(nok[0], jnp.logical_not(cross[0])), None, jnp.logical_and(nok[2], jnp.logical_not(cross[2]))]

    def greet(sem, *dev):
        pl.semaphore_signal(sem, inc=1, device_id=dev, device_id_type=MESH)

    barrier = pltpu.get_barrier_semaphore()
    for k in range(1, half):
        greet(barrier, w, zh * half + (within + k) % half)
    for i in (0, 2):
        @pl.when(wok[i])
        def _():
            greet(barrier, w + side(i), n)
        for j in (0, 2):
            @pl.when(jnp.logical_and(wok[i], same[j]))
            def _():
                greet(barrier, w + side(i), n + side(j))

    @pl.when(early)
    def _():
        greet(barrier, flip, zmate)
        for k in range(half):
            greet(barrier, w, half + (within + k) % half)

    for i in (0, 2):
        @pl.when(jnp.logical_and(wok[i], cross[2]))
        def _():
            greet(barrier, w + side(i), n + 1)

    def count(cond):
        return jnp.where(cond, jnp.int32(1), jnp.int32(0))

    wcount = count(wok[0]) + count(wok[2])
    expected = half - 1 + wcount * (1 + count(same[0]) + count(same[2]))
    expected = expected + count(late) * (half + 1) + count(cross[0]) * wcount

    @pl.when(n == 0)
    def _():
        fb[:, :, 0:256] = jnp.zeros((6, 64, 256), BF)
        pb[:, 0] = jnp.zeros((3, 128, 128), BF)

    @pl.when(n == nn - 1)
    def _():
        fb[:, :, 768:1024] = jnp.zeros((6, 64, 256), BF)
        pb[:, 2] = jnp.zeros((3, 128, 128), BF)

    @pl.when(w == 0)
    def _():
        fb[0:2] = jnp.zeros((2, 64, 1024), BF)
        pb[0] = jnp.zeros((3, 128, 128), BF)

    @pl.when(w == nw - 1)
    def _():
        fb[4:6] = jnp.zeros((2, 64, 1024), BF)
        pb[2] = jnp.zeros((3, 128, 128), BF)

    lane = lax.broadcasted_iota(jnp.int32, (1, 128), 1)

    def shifted(t, period):
        pos = lane % period
        before = jnp.where(pos > 0, pltpu.roll(t, 1, 1), 0.0)
        after = jnp.where(pos < period - 1, pltpu.roll(t, 127, 1), 0.0)
        return before.astype(BF), t.astype(BF), after.astype(BF)

    def stack1(d, h):
        t = fb[d, :, h * 128:(h + 1) * 128].astype(F32)
        for e, v in enumerate(shifted(t, 128)):
            xs1[d * 192 + e * 64:d * 192 + (e + 1) * 64, h * 128:(h + 1) * 128] = v

    eye = lax.broadcasted_iota(jnp.int32, (64, 64), 0) == lax.broadcasted_iota(jnp.int32, (64, 64), 1)

    def column(ref):
        return jnp.sum(jnp.where(eye, ref[...], 0.0), axis=1, keepdims=True)

    scale = column(sc_ref)
    shift = column(sh_ref)
    xf[...] = x_ref[...].astype(F32)
    for d in range(2):
        for h in range(4):
            t = xf[pl.ds(d * 4 + h, 64, stride=8), :]
            fb[2 + d, :, (2 + h) * 128:(3 + h) * 128] = (t * scale + shift).astype(BF)

    w3g[pl.ds(pl.multiple_of(n * 16, 16), 16), :] = w3_ref[...]

    pl.semaphore_wait(barrier, expected)

    @pl.when(late)
    def _():
        greet(fsem.at[1], flip, zmate)

    @pl.when(cross[0])
    def _():
        greet(fsem.at[0], w, n - 1)

    for k in range(half):
        @pl.when(jnp.logical_and(late, jnp.logical_or(n != half, k != half - 1)))
        def _():
            greet(fsem.at[2], w, (within + k) % half)

    for i in (0, 2):
        @pl.when(jnp.logical_and(wok[i], cross[0]))
        def _():
            greet(fsem.at[2], w + side(i), n - 1)

    def remote(src, dst, s, dev, r=None):
        return pltpu.make_async_remote_copy(
            src_ref=src, dst_ref=dst, send_sem=ssem.at[s], recv_sem=rsem.at[s if r is None else r],
            device_id=dev, device_id_type=MESH,
        )

    lo, hi = slice(256, 512), slice(512, 768)
    c_h = [
        remote(fb.at[2:4, :, lo], fb.at[2:4, :, 768:1024], H0, (w, n - 1)),
        remote(fb.at[2:4, :, hi], fb.at[2:4, :, 0:256], H0 + 1, (w, n + 1)),
    ]
    h_send = [nok[0], nok[2]]
    h_recv = [nok[2], nok[0]]
    own = slice(256, 768)
    c_d = [
        remote(fb.at[2:4, :, own], fb.at[4:6, :, own], D0, (w - 1, n)),
        remote(fb.at[2:4, :, own], fb.at[0:2, :, own], D0 + 1, (w + 1, n)),
    ]
    d_send = [wok[0], wok[2]]
    d_recv = [wok[2], wok[0]]
    edge = [slice(0, 256), slice(768, 1024)]
    c_g, g_send, g_recv = [], [], []
    for k, (dst, dev) in enumerate((((4, 6), w - 1), ((0, 2), w + 1))):
        for j in range(2):
            c_g.append(
                remote(fb.at[2:4, :, edge[j]], fb.at[dst[0]:dst[1], :, edge[j]], G0 + 2 * k + j, (dev, n))
            )
            g_send.append(jnp.logical_and(d_send[k], nok[2 * j]))
            g_recv.append(jnp.logical_and(d_recv[k], nok[2 * j]))

    def when(cond, f):
        pl.when(cond)(f)

    when(same[0], c_h[0].start)
    when(same[2], c_h[1].start)
    when(cross[0], c_h[0].start)
    for k in range(2):
        when(d_send[k], c_d[k].start)

    def shard(m):
        return w3g.at[pl.ds(pl.multiple_of(m * 16, 16), 16), :]

    c_wx = [remote(w3_ref, shard(n), WX0 + k - 1, (w, xmate(k))) for k in range(1, 4)]
    c_wz = remote(w3_ref, shard(n), WZ0, (flip, zmate))
    c_wf = [remote(shard(zmate), shard(zmate), WF0 + k - 1, (w, xmate(k))) for k in range(1, 4)]
    order = [n, xmate(1), xmate(2), xmate(3)]
    order = order + [(m + half) % nn for m in order]
    c_wc = [
        remote(w3_ref if k == 0 else shard(m), shard(m), WC0 + k, (w, mate))
        for k, m in enumerate(order)
    ]
    when(late, c_wz.start)
    for c in c_wx:
        c.start()
    c_wc[0].start()

    for a in range(3):
        for b in range(3):
            c0 = (a * 3 + b) * 192
            w1p[b * 64:(b + 1) * 64, a * 192:(a + 1) * 192] = w1_ref[:, c0:c0 + 192]
            w2p[b * 128:(b + 1) * 128, a * 192:(a + 1) * 192] = w2_ref[c0:c0 + 192, :].T
    for d in (2, 3):
        for h in range(2, 6):
            stack1(d, h)

    def edge_rows(depths, j):
        for d in depths:
            for h in ((0, 1), (6, 7))[j]:
                stack1(d, h)

    def forward(j, cond):
        for k in range(2):
            when(jnp.logical_and(cond, d_send[k]), c_g[2 * k + j].start)

    for j in range(2):
        when(same[2 * j], c_h[1 - j].wait_recv)
        forward(j, same[2 * j])
    @pl.when(cross[2])
    def _():
        pl.semaphore_wait(fsem.at[0], 1)
        c_h[1].start()

    @pl.when(early)
    def _():
        pl.semaphore_wait(fsem.at[1], 1)
        c_wz.start()

    for j in range(2):
        @pl.when(jnp.logical_not(cross[2 * j]))
        def _():
            edge_rows((2, 3), j)
    for k in range(2):
        when(d_recv[k], c_d[k].wait_recv)
    for d in (0, 1, 4, 5):
        for h in range(2, 6):
            stack1(d, h)
    for j in range(2):
        for k in range(2):
            when(jnp.logical_and(same[2 * j], d_recv[k]), c_g[2 * k + j].wait_recv)
        @pl.when(jnp.logical_not(cross[2 * j]))
        def _():
            edge_rows((0, 1, 4, 5), j)
    for j in range(2):
        @pl.when(cross[2 * j])
        def _():
            c_h[1 - j].wait_recv()
            forward(j, cross[2 * j])
            edge_rows((2, 3), j)
            for k in range(2):
                when(d_recv[k], c_g[2 * k + j].wait_recv)
            edge_rows((0, 1, 4, 5), j)

    def spread():
        c_wz.wait_recv()
        for c in c_wf:
            c.start()
        for k in range(3):
            c_wx[k].wait_recv()
        for k in range(1, 5):
            c_wc[k].start()

    when(cross[0], spread)

    lane6 = lax.broadcasted_iota(jnp.int32, (1, 768), 1)
    inside = jnp.logical_and(
        jnp.logical_or(lane6 >= 128, n > 0), jnp.logical_or(lane6 < 640, n < nn - 1)
    )

    def first(d, carry):
        y = jnp.dot(
            w1p[...], xs1[pl.ds(pl.multiple_of(d * 192, 192), 576), :], preferred_element_type=F32
        )
        y = y[0:64, 0:768] + y[64:128, 128:896] + y[128:192, 256:1024]
        level = 2 * w + d - 1
        keep = jnp.logical_and(inside, jnp.logical_and(level >= 0, level < 2 * nw))
        y = jnp.where(keep, jnp.maximum(y, 0.0), 0.0)
        for h in range(6):
            for e, v in enumerate(shifted(y[:, h * 128:(h + 1) * 128], 128)):
                xs2[pl.ds(pl.multiple_of(d * 192 + e * 64, 64), 64), h * 128:(h + 1) * 128] = v
        return carry

    lax.fori_loop(0, 4, first, 0)

    def second(d):
        y = jnp.dot(w2p[...], xs2[d * 192:d * 192 + 576, :], preferred_element_type=F32)
        return y[0:128, 0:512] + y[128:256, 128:640] + y[256:384, 256:768]

    s = jnp.maximum(jnp.maximum(second(0), second(1)), 0.0)
    rows = []
    for r in range(2):
        t = jnp.maximum(s[:, r * 256:r * 256 + 128], s[:, r * 256 + 128:r * 256 + 256])
        rows.append(jnp.maximum(t, pltpu.roll(t, 127, 1)).astype(BF))
    k_i = lax.broadcasted_iota(jnp.int32, (128, 128), 0)
    j_i = lax.broadcasted_iota(jnp.int32, (128, 128), 1)
    pick0 = jnp.where(k_i == 2 * j_i, 1.0, 0.0).astype(BF)
    pick1 = jnp.where(k_i == 2 * (j_i - 64), 1.0, 0.0).astype(BF)
    pooled = jnp.dot(rows[0], pick0, preferred_element_type=F32) + jnp.dot(
        rows[1], pick1, preferred_element_type=F32
    )
    pb[1, 1] = pooled.astype(BF)

    @pl.when(early)
    def _():
        pl.semaphore_wait(fsem.at[2], half - count(cross[2]) + count(cross[2]) * wcount)

    c_p = []
    for k, (i, j) in enumerate(near):
        c_p.append(
            remote(pb.at[1, 1], pb.at[2 - i, 2 - j], P0 + k, (w + side(i), n + side(j)))
        )
        when(ok(i, j), c_p[k].start)

    when(jnp.logical_not(cross[0]), spread)
    for c in c_wf:
        c.wait_recv()
    for k in range(5, 8):
        c_wc[k].start()

    for k, (i, j) in enumerate(near):
        when(ok(2 - i, 2 - j), c_p[k].wait_recv)

    low = lane < 64

    def coarse_stack(a, carry):
        left = pb[a, 0].astype(F32)
        mid = pb[a, 1].astype(F32)
        right = pb[a, 2].astype(F32)
        tops = (
            pltpu.roll(jnp.where(low, mid, left), 64, 1),
            mid,
            pltpu.roll(jnp.where(low, right, mid), 64, 1),
        )
        for b, t in enumerate(tops):
            for e, v in enumerate(shifted(t, 64)):
                xs3[pl.ds(pl.multiple_of(a * 1152 + (b * 3 + e) * 128, 128), 128), :] = v
        return carry

    lax.fori_loop(0, 3, coarse_stack, 0)

    for c in c_wc:
        c.wait_recv()

    def coarse(g, carry):
        y = jnp.dot(
            w3g[pl.ds(pl.multiple_of(g * 128, 128), 128), :], xs3[...], preferred_element_type=F32
        )
        ob[pl.ds(pl.multiple_of(g * 128, 128), 128), :] = jnp.maximum(y, 0.0).astype(BF)
        return carry

    lax.fori_loop(0, 2, coarse, 0)

    def block(m):
        return out_ref.at[:, pl.ds(pl.multiple_of(m * 128, 128), 128)]

    def piece(m):
        return ob.at[pl.ds(pl.multiple_of(m * 16, 16), 16), :]

    c_a = []
    for k in range(1, nn):
        m = (n + k) % nn
        c = remote(piece(m), block(n), A0 + k, (w, m))
        c.start()
        c_a.append(c)
    out_ref[:, pl.ds(pl.multiple_of(n * 128, 128), 128)] = ob[
        pl.ds(pl.multiple_of(n * 16, 16), 16), :
    ]

    for k in range(1, nn):
        src = (n - k + nn) % nn
        remote(piece(n), block(src), A0 + k, (w, src)).wait_recv()

    for k in range(2):
        when(h_send[k], c_h[k].wait_send)
        when(d_send[k], c_d[k].wait_send)
    for k in range(4):
        when(g_send[k], c_g[k].wait_send)
    for k, (i, j) in enumerate(near):
        when(ok(i, j), c_p[k].wait_send)
    c_wz.wait_send()
    for c in c_wx + c_wf + c_wc + c_a:
        c.wait_send()


def solution(mesh):
    nw, nn = mesh.shape["wide"], mesh.shape["narrow"]

    def body(stored_features, channel_scale, channel_shift, first_weight, second_weight, third_weight):
        x = stored_features.reshape(512, 128)
        out = pl.pallas_call(
            functools.partial(kernel, nw, nn),
            out_shape=pltpu.VMEM((16, nn * 128), BF),
            in_specs=[pl.BlockSpec(memory_space=pltpu.VMEM)] * 6,
            out_specs=pl.BlockSpec(memory_space=pltpu.VMEM),
            scratch_shapes=[
                pltpu.VMEM((512, 128), F32),
                pltpu.VMEM((6, 64, 1024), BF),
                pltpu.VMEM((6 * 192, 1024), BF),
                pltpu.VMEM((4 * 192, 768), BF),
                pltpu.VMEM((192, 576), BF),
                pltpu.VMEM((384, 576), BF),
                pltpu.VMEM((3, 3, 128, 128), BF),
                pltpu.VMEM((3456, 128), BF),
                pltpu.VMEM((nn * 16, 3456), BF),
                pltpu.VMEM((256, 128), BF),
                pltpu.SemaphoreType.DMA((NSEM,)),
                pltpu.SemaphoreType.DMA((NSEM,)),
                pltpu.SemaphoreType.REGULAR((3,)),
            ],
            compiler_params=pltpu.CompilerParams(collective_id=0, has_side_effects=True),
        )(x, channel_scale.reshape(1, 64), channel_shift.reshape(1, 64), first_weight, second_weight.T, third_weight)
        return out.reshape(16, 1, nn * 128)

    in_specs = (P(None, "wide", "narrow", None), P(), P(), P(), P(), P("narrow", None))
    return jax.shard_map(
        body, mesh=mesh, in_specs=in_specs, out_specs=P("narrow", "wide", None), check_vma=False
    )
```

```python
import functools

import jax
import jax.numpy as jnp
from jax import lax
from jax.experimental import pallas as pl
from jax.experimental.pallas import tpu as pltpu
from jax.sharding import PartitionSpec as P

BF = jnp.bfloat16
F32 = jnp.float32
MESH = pl.DeviceIdType.MESH
SPREAD = 0

names = dict(H=2, D=2, G=4, P=8, WX=3, WZ=2, WF=6, WC=8, A=16, X=3, E=2, B=16, L=6)
BASE, NSEM = {}, 0
for name, size in names.items():
    BASE[name] = NSEM
    NSEM += size
H0, D0, G0, P0, WX0, WZ0, WF0, WC0, A0, X0, E0, B0, L0 = BASE.values()


def kernel(nw, nn, x_hbm, sc_hbm, sh_hbm, w1_hbm, w2_hbm, w3_hbm, out_ref,
           x_ref, sc_ref, sh_ref, w1_ref, w2_ref, xf, fb, xs1, xs2, w1p, w2p, pb, xs3, w3g, ob, rb, xs4, of, px, ssem, rsem, fsem):
    w = lax.axis_index("wide")
    n = lax.axis_index("narrow")
    half = nn // 2
    zh = n // half
    within = n % half
    mate = n + 1 - 2 * (n % 2)
    zmate = (n + half) % nn

    def xmate(k):
        return zh * half + (within + 2 * k) % half

    def side(i):
        return i - 1

    wok = [w > 0, None, w < nw - 1]
    nok = [n > 0, None, n < nn - 1]

    def ok(i, j):
        if i == 1:
            return nok[j]
        if j == 1:
            return wok[i]
        return jnp.logical_and(wok[i], nok[j])

    near = [(i, j) for i in range(3) for j in range(3) if (i, j) != (1, 1)]

    early = zh == 0
    late = zh == 1
    flip = (nw // 8 - 1 - w // 8) * 8 + w % 8 if nw % 8 == 0 else w
    cross = [jnp.logical_and(n == half, late), None, jnp.logical_and(n == half - 1, early)]
    same = [jnp.logical_and(nok[0], jnp.logical_not(cross[0])), None, jnp.logical_and(nok[2], jnp.logical_not(cross[2]))]

    def greet(sem, *dev):
        pl.semaphore_signal(sem, inc=1, device_id=dev, device_id_type=MESH)

    barrier = pltpu.get_barrier_semaphore()
    for k in range(1, half):
        greet(barrier, w, zh * half + (within + k) % half)
    for i in (0, 2):
        @pl.when(wok[i])
        def _():
            greet(barrier, w + side(i), n)
        for j in (0, 2):
            @pl.when(jnp.logical_and(wok[i], same[j]))
            def _():
                greet(barrier, w + side(i), n + side(j))

    @pl.when(early)
    def _():
        greet(barrier, flip, zmate)
        for k in range(half):
            greet(barrier, w, half + (within + k) % half)

    def count(cond):
        return jnp.where(cond, jnp.int32(1), jnp.int32(0))

    wcount = count(wok[0]) + count(wok[2])
    expected = half - 1 + wcount * (1 + count(same[0]) + count(same[2]))
    expected = expected + count(late) * (half + 1)

    mine = pl.ds(pl.multiple_of(n * 16, 16), 16)
    loads = [
        pltpu.make_async_copy(src, dst, rsem.at[L0 + k])
        for k, (src, dst) in enumerate((
            (x_hbm, x_ref), (sc_hbm, sc_ref), (sh_hbm, sh_ref),
            (w3_hbm, w3g.at[mine, :]), (w1_hbm, w1_ref), (w2_hbm, w2_ref),
        ))
    ]
    for c in loads:
        c.start()

    @pl.when(jnp.logical_or(n == 0, n == half))
    def _():
        fb[:, :, 0:256] = jnp.zeros((6, 64, 256), BF)
        pb[:, 0] = jnp.zeros((3, 128, 128), BF)

    @pl.when(n == nn - 1)
    def _():
        fb[:, :, 768:1024] = jnp.zeros((6, 64, 256), BF)
        pb[:, 2] = jnp.zeros((3, 128, 128), BF)

    @pl.when(w == 0)
    def _():
        fb[0:2] = jnp.zeros((2, 64, 1280), BF)
        pb[0] = jnp.zeros((3, 128, 128), BF)

    @pl.when(w == nw - 1)
    def _():
        fb[4:6] = jnp.zeros((2, 64, 1280), BF)
        pb[2] = jnp.zeros((3, 128, 128), BF)

    lane = lax.broadcasted_iota(jnp.int32, (1, 128), 1)

    def shifted(t, period):
        pos = lane % period
        before = jnp.where(pos > 0, pltpu.roll(t, 1, 1), 0.0)
        after = jnp.where(pos < period - 1, pltpu.roll(t, 127, 1), 0.0)
        return before.astype(BF), t.astype(BF), after.astype(BF)

    def stack1(d, h):
        t = fb[d, :, h * 128:(h + 1) * 128].astype(F32)
        for e, v in enumerate(shifted(t, 128)):
            xs1[d * 192 + e * 64:d * 192 + (e + 1) * 64, h * 128:(h + 1) * 128] = v

    eye = lax.broadcasted_iota(jnp.int32, (64, 64), 0) == lax.broadcasted_iota(jnp.int32, (64, 64), 1)

    def column(ref):
        return jnp.sum(jnp.where(eye, ref[...], 0.0), axis=1, keepdims=True)

    for c in loads[:3]:
        c.wait()
    scale = column(sc_ref)
    shift = column(sh_ref)
    xf[...] = x_ref[...].astype(F32)
    for d in range(2):
        for h in range(4):
            t = xf[pl.ds(d * 4 + h, 64, stride=8), :]
            fb[2 + d, :, (2 + h) * 128:(3 + h) * 128] = (t * scale + shift).astype(BF)

    loads[3].wait()
    pl.semaphore_wait(barrier, expected)

    @pl.when(late)
    def _():
        greet(fsem.at[0], flip, zmate)
        for k in range(half):
            greet(fsem.at[1], w, (within + k) % half)

    def remote(src, dst, s, dev, r=None):
        return pltpu.make_async_remote_copy(
            src_ref=src, dst_ref=dst, send_sem=ssem.at[s], recv_sem=rsem.at[s if r is None else r],
            device_id=dev, device_id_type=MESH,
        )

    lo, hi = slice(256, 512), slice(512, 768)
    c_h = [
        remote(fb.at[2:4, :, lo], fb.at[2:4, :, 768:1024], H0, (w, n - 1)),
        remote(fb.at[2:4, :, hi], fb.at[2:4, :, 0:256], H0 + 1, (w, n + 1)),
    ]
    own = slice(256, 768)
    c_d = [
        remote(fb.at[2:4, :, own], fb.at[4:6, :, own], D0, (w - 1, n)),
        remote(fb.at[2:4, :, own], fb.at[0:2, :, own], D0 + 1, (w + 1, n)),
    ]
    d_send = [wok[0], wok[2]]
    d_recv = [wok[2], wok[0]]
    edge = [slice(0, 256), slice(768, 1024)]
    c_g, g_send, g_recv = [], [], []
    for k, (dst, dev) in enumerate((((4, 6), w - 1), ((0, 2), w + 1))):
        for j in range(2):
            c_g.append(
                remote(fb.at[2:4, :, edge[j]], fb.at[dst[0]:dst[1], :, edge[j]], G0 + 2 * k + j, (dev, n))
            )
            g_send.append(jnp.logical_and(d_send[k], same[2 * j]))
            g_recv.append(jnp.logical_and(d_recv[k], same[2 * j]))

    far = slice(768, 1280)
    c_x = [
        remote(fb.at[2:4, :, own], fb.at[2:4, :, far], X0, (w, n - 1)),
        remote(fb.at[2:4, :, far], fb.at[4:6, :, far], X0 + 1, (w - 1, n)),
        remote(fb.at[2:4, :, far], fb.at[0:2, :, far], X0 + 2, (w + 1, n)),
    ]

    def when(cond, f):
        pl.when(cond)(f)

    upper = cross[2]
    lower = cross[0]
    when(lower, c_x[0].start)
    when(same[0], c_h[0].start)
    when(same[2], c_h[1].start)
    for k in range(2):
        when(d_send[k], c_d[k].start)

    def shard(m):
        return w3g.at[pl.ds(pl.multiple_of(m * 16, 16), 16), :]

    c_wx = [remote(shard(n), shard(n), WX0 + k - 1, (w, xmate(k))) for k in range(1, 4)]

    def half_shard(m, q):
        return w3g.at[pl.ds(pl.multiple_of(m * 16, 16), 16), (slice(0, 1792), slice(1792, 3456))[q]]

    c_wz = [remote(half_shard(n, q), half_shard(n, q), WZ0 + q, (flip, zmate)) for q in range(2)]
    c_wf = [
        [
            remote(half_shard(zmate, q), half_shard(zmate, q), WF0 + 3 * q + k - 1, (w, xmate(k)))
            for k in range(1, 4)
        ]
        for q in range(2)
    ]
    order = [n, xmate(1), xmate(2), xmate(3)]
    order = order + [(m + half) % nn for m in order]
    c_wc = [remote(shard(m), shard(m), WC0 + k, (w, mate)) for k, m in enumerate(order)]
    for q in range(2):
        when(late, c_wz[q].start)
    for c in c_wx:
        c.start()
    c_wc[0].start()

    loads[4].wait()
    loads[5].wait()
    for a in range(3):
        for b in range(3):
            c0 = (a * 3 + b) * 192
            w1p[b * 64:(b + 1) * 64, a * 192:(a + 1) * 192] = w1_ref[:, c0:c0 + 192]
            w2p[b * 128:(b + 1) * 128, a * 192:(a + 1) * 192] = w2_ref[c0:c0 + 192, :].T
    for d in (2, 3):
        for h in range(2, 6):
            stack1(d, h)

    def edge_rows(depths, j):
        for d in depths:
            for h in ((0, 1), (6, 7))[j]:
                stack1(d, h)

    def forward(j, cond):
        for k in range(2):
            when(jnp.logical_and(cond, d_send[k]), c_g[2 * k + j].start)

    for j in range(2):
        when(same[2 * j], c_h[1 - j].wait_recv)
        forward(j, same[2 * j])
    @pl.when(early)
    def _():
        pl.semaphore_wait(fsem.at[0], 1)
        for c in c_wz:
            c.start()

    edge_rows((2, 3), 0)
    when(jnp.logical_not(upper), lambda: edge_rows((2, 3), 1))
    for k in range(2):
        when(d_recv[k], c_d[k].wait_recv)
    for d in (0, 1, 4, 5):
        for h in range(2, 6):
            stack1(d, h)
    for k in range(4):
        when(g_recv[k], c_g[k].wait_recv)
    edge_rows((0, 1, 4, 5), 0)
    when(jnp.logical_not(upper), lambda: edge_rows((0, 1, 4, 5), 1))

    def spread():
        for q in range(2):
            c_wz[q].wait_recv()
            for c in c_wf[q]:
                c.start()
        for k in range(3):
            c_wx[k].wait_recv()
        for k in range(1, 5):
            c_wc[k].start()

    def first(h0, rows):
        row = h0 * 128 + lax.broadcasted_iota(jnp.int32, (1, rows * 128), 1)
        inside = jnp.logical_and(
            jnp.logical_or(row >= 128, n > 0), jnp.logical_or(row < 640, n < nn - 1)
        )
        span = rows * 128

        def level(d, carry):
            y = jnp.dot(
                w1p[...],
                xs1[pl.ds(pl.multiple_of(d * 192, 192), 576), h0 * 128:h0 * 128 + span + 256],
                preferred_element_type=F32,
            )
            y = y[0:64, 0:span] + y[64:128, 128:span + 128] + y[128:192, 256:span + 256]
            depth = 2 * w + d - 1
            keep = jnp.logical_and(inside, jnp.logical_and(depth >= 0, depth < 2 * nw))
            y = jnp.where(keep, jnp.maximum(y, 0.0), 0.0)
            for h in range(rows):
                for e, v in enumerate(shifted(y[:, h * 128:(h + 1) * 128], 128)):
                    c0 = (h0 + h) * 128
                    xs2[pl.ds(pl.multiple_of(d * 192 + e * 64, 64), 64), c0:c0 + 128] = v
            return carry

        lax.fori_loop(0, 4, level, 0)

    def second(h0, rows):
        span = rows * 128

        def level(d):
            y = jnp.dot(
                w2p[...], xs2[d * 192:d * 192 + 576, h0 * 128:h0 * 128 + span + 256],
                preferred_element_type=F32,
            )
            return y[0:128, 0:span] + y[128:256, 128:span + 128] + y[256:384, 256:span + 256]

        s = jnp.maximum(jnp.maximum(level(0), level(1)), 0.0)
        out = []
        for r in range(rows // 2):
            t = jnp.maximum(s[:, r * 256:r * 256 + 128], s[:, r * 256 + 128:r * 256 + 256])
            out.append(jnp.maximum(t, pltpu.roll(t, 127, 1)).astype(BF))
        return out

    k_i = lax.broadcasted_iota(jnp.int32, (128, 128), 0)
    j_i = lax.broadcasted_iota(jnp.int32, (128, 128), 1)

    def pick(t, place):
        cells = jnp.where(k_i == 2 * (j_i - 64 * place), 1.0, 0.0).astype(BF)
        return jnp.dot(t, cells, preferred_element_type=F32)

    @pl.when(jnp.logical_not(upper))
    def _():
        if SPREAD == 0:
            spread()
        first(0, 6)
        if SPREAD == 1:
            spread()
        r0, r1 = second(0, 4)
        keep = jnp.where(lower, 0.0, 1.0)
        pb[1, 1] = (pick(r0, 0) * keep + pick(r1, 1)).astype(BF)

    @pl.when(upper)
    def _():
        c_x[0].wait_recv()
        for k in range(2):
            when(d_send[k], c_x[1 + k].start)
        if SPREAD == 0:
            spread()
        for d in (2, 3):
            for h in range(6, 10):
                stack1(d, h)
        first(0, 4)
        if SPREAD == 1:
            spread()
        rb[...] = second(0, 2)[0]
        for k in range(2):
            when(d_recv[k], c_x[1 + k].wait_recv)
        for d in (0, 1, 4, 5):
            for h in range(6, 10):
                stack1(d, h)
        first(4, 4)
        r1, r2 = second(2, 4)
        pb[1, 1] = (pick(rb[...], 0) + pick(r1, 1)).astype(BF)
        pb[1, 2] = pick(r2, 0).astype(BF)

    def beside(i, j):
        if j == 1:
            return wok[i]
        if i == 1:
            return same[j]
        return jnp.logical_and(wok[i], same[j])

    c_e = [
        remote(pb.at[1, 2], pb.at[2, 2], E0, (w - 1, n)),
        remote(pb.at[1, 2], pb.at[0, 2], E0 + 1, (w + 1, n)),
    ]
    for k in range(2):
        when(jnp.logical_and(upper, d_send[k]), c_e[k].start)
    c_p = []
    for k, (i, j) in enumerate(near):
        c_p.append(
            remote(pb.at[1, 1], pb.at[2 - i, 2 - j], P0 + k, (w + side(i), n + side(j)))
        )
        when(beside(i, j), c_p[k].start)

    if SPREAD == 2:
        spread()
    for c in c_wf[0] + c_wf[1]:
        c.wait_recv()
    for k in range(5, 8):
        c_wc[k].start()

    for k, (i, j) in enumerate(near):
        when(beside(2 - i, 2 - j), c_p[k].wait_recv)

    low = lane < 64

    @pl.when(upper)
    def _():
        for k in range(2):
            when(d_recv[k], c_e[k].wait_recv)

    def coarse_stack(left_of, mid_of, right_of, dst):
        def level(a, carry):
            left = left_of(a).astype(F32)
            mid = mid_of(a).astype(F32)
            right = right_of(a).astype(F32)
            tops = (
                pltpu.roll(jnp.where(low, mid, left), 64, 1),
                mid,
                pltpu.roll(jnp.where(low, right, mid), 64, 1),
            )
            for b, t in enumerate(tops):
                for e, v in enumerate(shifted(t, 64)):
                    dst[pl.ds(pl.multiple_of(a * 1152 + (b * 3 + e) * 128, 128), 128), :] = v
            return carry

        lax.fori_loop(0, 3, level, 0)

    coarse_stack(lambda a: pb[a, 0], lambda a: pb[a, 1], lambda a: pb[a, 2], xs3)
    blank = jnp.zeros((128, 128), F32)
    when(upper, lambda: coarse_stack(lambda a: pb[a, 1], lambda a: pb[a, 2], lambda a: blank, xs4))

    for c in c_wc:
        c.wait_recv()

    def coarse(src, whole):
        def part(g, carry):
            rows = pl.ds(pl.multiple_of(g * 128, 128), 128)
            y = jnp.dot(w3g[rows, :], src[...], preferred_element_type=F32)
            if whole:
                ob[rows, :] = jnp.maximum(y, 0.0).astype(BF)
            else:
                of[rows, :] = y
            return carry

        lax.fori_loop(0, 2, part, 0)

    when(jnp.logical_not(lower), lambda: coarse(xs3, True))
    when(lower, lambda: coarse(xs3, False))
    when(upper, lambda: coarse(xs4, False))

    @pl.when(early)
    def _():
        pl.semaphore_wait(fsem.at[1], half)

    def block(m):
        return out_ref.at[:, pl.ds(pl.multiple_of(m * 128, 128), 128)]

    def piece(ref, m):
        return ref.at[pl.ds(pl.multiple_of(m * 16, 16), 16), :]

    c_a, c_b = [], []
    for k in range(1, nn):
        m = (n + k) % nn
        c_a.append(remote(piece(ob, m), block(n), A0 + k, (w, m)))
        c_b.append([
            remote(piece(of, m), px.at[q], B0 + k, (w, m), r=B0 + q) for q in range(2)
        ])
        when(jnp.logical_not(lower), c_a[-1].start)
        when(upper, c_b[-1][0].start)
        when(lower, c_b[-1][1].start)

    @pl.when(jnp.logical_not(lower))
    def _():
        out_ref[:, pl.ds(pl.multiple_of(n * 128, 128), 128)] = ob[mine, :]

    @pl.when(upper)
    def _():
        px[0] = of[mine, :]

    @pl.when(lower)
    def _():
        px[1] = of[mine, :]

    for k in range(1, nn):
        src = (n - k + nn) % nn
        when(src != half, remote(piece(ob, n), block(src), A0 + k, (w, src)).wait_recv)
    for q, home in enumerate((upper, lower)):
        when(jnp.logical_not(home), remote(piece(of, n), px.at[q], B0 + q, (w, half - 1 + q)).wait_recv)
    out_ref[:, half * 128:(half + 1) * 128] = jnp.maximum(px[0] + px[1], 0.0).astype(BF)

    when(same[0], c_h[0].wait_send)
    when(same[2], c_h[1].wait_send)
    for k in range(2):
        when(d_send[k], c_d[k].wait_send)
    for k in range(4):
        when(g_send[k], c_g[k].wait_send)
    for k, (i, j) in enumerate(near):
        when(beside(i, j), c_p[k].wait_send)
    for c in c_wz + c_wx + c_wf[0] + c_wf[1] + c_wc:
        c.wait_send()

    @pl.when(lower)
    def _():
        c_x[0].wait_send()
        for c in c_b:
            c[1].wait_send()

    @pl.when(upper)
    def _():
        for k in range(2):
            when(d_send[k], c_x[1 + k].wait_send)
            when(d_send[k], c_e[k].wait_send)
        for c in c_b:
            c[0].wait_send()

    @pl.when(jnp.logical_not(lower))
    def _():
        for c in c_a:
            c.wait_send()


def solution(mesh):
    nw, nn = mesh.shape["wide"], mesh.shape["narrow"]

    def body(stored_features, channel_scale, channel_shift, first_weight, second_weight, third_weight):
        x = stored_features.reshape(512, 128)
        out = pl.pallas_call(
            functools.partial(kernel, nw, nn),
            out_shape=pltpu.VMEM((16, nn * 128), BF),
            in_specs=[pl.BlockSpec(memory_space=pl.ANY)] * 6,
            out_specs=pl.BlockSpec(memory_space=pltpu.VMEM),
            scratch_shapes=[
                pltpu.VMEM((512, 128), BF),
                pltpu.VMEM((1, 64), F32),
                pltpu.VMEM((1, 64), F32),
                pltpu.VMEM((64, 1728), BF),
                pltpu.VMEM((1728, 128), BF),
                pltpu.VMEM((512, 128), F32),
                pltpu.VMEM((6, 64, 1280), BF),
                pltpu.VMEM((6 * 192, 1280), BF),
                pltpu.VMEM((4 * 192, 1024), BF),
                pltpu.VMEM((192, 576), BF),
                pltpu.VMEM((384, 576), BF),
                pltpu.VMEM((3, 3, 128, 128), BF),
                pltpu.VMEM((3456, 128), BF),
                pltpu.VMEM((nn * 16, 3456), BF),
                pltpu.VMEM((256, 128), BF),
                pltpu.VMEM((128, 128), BF),
                pltpu.VMEM((3456, 128), BF),
                pltpu.VMEM((256, 128), F32),
                pltpu.VMEM((2, 16, 128), F32),
                pltpu.SemaphoreType.DMA((NSEM,)),
                pltpu.SemaphoreType.DMA((NSEM,)),
                pltpu.SemaphoreType.REGULAR((2,)),
            ],
            compiler_params=pltpu.CompilerParams(collective_id=0, has_side_effects=True),
        )(x, channel_scale.reshape(1, 64), channel_shift.reshape(1, 64), first_weight, second_weight.T, third_weight)
        return out.reshape(16, 1, nn * 128)

    in_specs = (P(None, "wide", "narrow", None), P(), P(), P(), P(), P("narrow", None))
    return jax.shard_map(
        body, mesh=mesh, in_specs=in_specs, out_specs=P("narrow", "wide", None), check_vma=False
    )
```

```python
import functools

import jax
import jax.numpy as jnp
from jax import lax
from jax.experimental import pallas as pl
from jax.experimental.pallas import tpu as pltpu
from jax.sharding import PartitionSpec as P

BF = jnp.bfloat16
F32 = jnp.float32
MESH = pl.DeviceIdType.MESH
SPREAD = 0

names = dict(H=2, D=2, G=4, P=8, WX=3, WZ=2, WF=6, WC=8, A=16, X=3, E=2, B=16, L=6)
BASE, NSEM = {}, 0
for name, size in names.items():
    BASE[name] = NSEM
    NSEM += size
H0, D0, G0, P0, WX0, WZ0, WF0, WC0, A0, X0, E0, B0, L0 = BASE.values()


def kernel(nw, nn, x_hbm, sc_hbm, sh_hbm, w1_hbm, w2_hbm, w3_hbm, out_ref,
           x_ref, sc_ref, sh_ref, w1_ref, w2_ref, xf, fb, xs1, xs2, w1p, w2p, pb, xs3, w3g, ob, rb, xs4, of, px, ssem, rsem, fsem):
    w = lax.axis_index("wide")
    n = lax.axis_index("narrow")
    half = nn // 2
    zh = n // half
    within = n % half
    mate = n + 1 - 2 * (n % 2)
    zmate = (n + half) % nn

    def xmate(k):
        return zh * half + (within + 2 * k) % half

    def side(i):
        return i - 1

    wok = [w > 0, None, w < nw - 1]
    nok = [n > 0, None, n < nn - 1]

    def ok(i, j):
        if i == 1:
            return nok[j]
        if j == 1:
            return wok[i]
        return jnp.logical_and(wok[i], nok[j])

    near = [(i, j) for i in range(3) for j in range(3) if (i, j) != (1, 1)]

    early = zh == 0
    late = zh == 1
    flip = (nw // 8 - 1 - w // 8) * 8 + w % 8 if nw % 8 == 0 else w
    cross = [jnp.logical_and(n == half, late), None, jnp.logical_and(n == half - 1, early)]
    same = [jnp.logical_and(nok[0], jnp.logical_not(cross[0])), None, jnp.logical_and(nok[2], jnp.logical_not(cross[2]))]

    def greet(sem, *dev):
        pl.semaphore_signal(sem, inc=1, device_id=dev, device_id_type=MESH)

    barrier = pltpu.get_barrier_semaphore()
    for k in range(1, half):
        greet(barrier, w, zh * half + (within + k) % half)
    for i in (0, 2):
        @pl.when(wok[i])
        def _():
            greet(barrier, w + side(i), n)
        for j in (0, 2):
            @pl.when(jnp.logical_and(wok[i], same[j]))
            def _():
                greet(barrier, w + side(i), n + side(j))

    @pl.when(early)
    def _():
        greet(barrier, flip, zmate)
        for k in range(half):
            greet(barrier, w, half + (within + k) % half)

    def count(cond):
        return jnp.where(cond, jnp.int32(1), jnp.int32(0))

    wcount = count(wok[0]) + count(wok[2])
    expected = half - 1 + wcount * (1 + count(same[0]) + count(same[2]))
    expected = expected + count(late) * (half + 1)

    mine = pl.ds(pl.multiple_of(n * 16, 16), 16)
    loads = [
        pltpu.make_async_copy(src, dst, rsem.at[L0 + k])
        for k, (src, dst) in enumerate((
            (x_hbm, x_ref), (sc_hbm, sc_ref), (sh_hbm, sh_ref),
            (w3_hbm, w3g.at[mine, :]), (w1_hbm, w1_ref), (w2_hbm, w2_ref),
        ))
    ]
    for c in loads:
        c.start()

    @pl.when(jnp.logical_or(n == 0, n == half))
    def _():
        fb[:, :, 0:256] = jnp.zeros((6, 64, 256), BF)
        pb[:, 0] = jnp.zeros((3, 64, 128), BF)

    @pl.when(n == nn - 1)
    def _():
        fb[:, :, 768:1024] = jnp.zeros((6, 64, 256), BF)
        pb[:, 3] = jnp.zeros((3, 64, 128), BF)

    @pl.when(w == 0)
    def _():
        fb[0:2] = jnp.zeros((2, 64, 1280), BF)
        pb[0] = jnp.zeros((4, 64, 128), BF)

    @pl.when(w == nw - 1)
    def _():
        fb[4:6] = jnp.zeros((2, 64, 1280), BF)
        pb[2] = jnp.zeros((4, 64, 128), BF)

    lane = lax.broadcasted_iota(jnp.int32, (1, 128), 1)

    def shifted(t, period):
        pos = lane % period
        before = jnp.where(pos > 0, pltpu.roll(t, 1, 1), 0.0)
        after = jnp.where(pos < period - 1, pltpu.roll(t, 127, 1), 0.0)
        return before.astype(BF), t.astype(BF), after.astype(BF)

    def stack1(d, h):
        t = fb[d, :, h * 128:(h + 1) * 128].astype(F32)
        for e, v in enumerate(shifted(t, 128)):
            xs1[d * 192 + e * 64:d * 192 + (e + 1) * 64, h * 128:(h + 1) * 128] = v

    eye = lax.broadcasted_iota(jnp.int32, (64, 64), 0) == lax.broadcasted_iota(jnp.int32, (64, 64), 1)

    def column(ref):
        return jnp.sum(jnp.where(eye, ref[...], 0.0), axis=1, keepdims=True)

    for c in loads[:3]:
        c.wait()
    scale = column(sc_ref)
    shift = column(sh_ref)
    xf[...] = x_ref[...].astype(F32)
    for d in range(2):
        for h in range(4):
            t = xf[pl.ds(d * 4 + h, 64, stride=8), :]
            fb[2 + d, :, (2 + h) * 128:(3 + h) * 128] = (t * scale + shift).astype(BF)

    loads[3].wait()
    pl.semaphore_wait(barrier, expected)

    @pl.when(late)
    def _():
        greet(fsem.at[0], flip, zmate)
        for k in range(half):
            greet(fsem.at[1], w, (within + k) % half)

    def remote(src, dst, s, dev, r=None):
        return pltpu.make_async_remote_copy(
            src_ref=src, dst_ref=dst, send_sem=ssem.at[s], recv_sem=rsem.at[s if r is None else r],
            device_id=dev, device_id_type=MESH,
        )

    lo, hi = slice(256, 512), slice(512, 768)
    c_h = [
        remote(fb.at[2:4, :, lo], fb.at[2:4, :, 768:1024], H0, (w, n - 1)),
        remote(fb.at[2:4, :, hi], fb.at[2:4, :, 0:256], H0 + 1, (w, n + 1)),
    ]
    own = slice(256, 768)
    c_d = [
        remote(fb.at[2:4, :, own], fb.at[4:6, :, own], D0, (w - 1, n)),
        remote(fb.at[2:4, :, own], fb.at[0:2, :, own], D0 + 1, (w + 1, n)),
    ]
    d_send = [wok[0], wok[2]]
    d_recv = [wok[2], wok[0]]
    even = n % 2 == 0
    outer = jnp.logical_or(jnp.logical_and(even, same[0]), jnp.logical_and(jnp.logical_not(even), same[2]))

    def rows_at(on_even, on_odd):
        return pl.ds(pl.multiple_of(jnp.where(even, on_even, on_odd), 256), 256)

    outside = rows_at(0, 768)
    c_g = [
        remote(fb.at[2:4, :, outside], fb.at[4:6, :, outside], G0, (w - 1, n)),
        remote(fb.at[2:4, :, outside], fb.at[0:2, :, outside], G0 + 1, (w + 1, n)),
    ]
    depths = (slice(4, 6), slice(0, 2))
    c_i = [
        remote(fb.at[depths[k], :, rows_at(512, 256)], fb.at[depths[k], :, rows_at(0, 768)], G0 + 2 + k, (w, mate))
        for k in range(2)
    ]
    far = slice(768, 1280)
    c_x = [
        remote(fb.at[2:4, :, own], fb.at[2:4, :, far], X0, (w, n - 1)),
        remote(fb.at[2:4, :, far], fb.at[4:6, :, far], X0 + 1, (w - 1, n)),
        remote(fb.at[2:4, :, far], fb.at[0:2, :, far], X0 + 2, (w + 1, n)),
    ]

    def when(cond, f):
        pl.when(cond)(f)

    upper = cross[2]
    lower = cross[0]
    when(lower, c_x[0].start)
    when(same[0], c_h[0].start)
    when(same[2], c_h[1].start)
    for k in range(2):
        when(d_send[k], c_d[k].start)

    def shard(m):
        return w3g.at[pl.ds(pl.multiple_of(m * 16, 16), 16), :]

    c_wx = [remote(shard(n), shard(n), WX0 + k - 1, (w, xmate(k))) for k in range(1, 4)]

    def half_shard(m, q):
        return w3g.at[pl.ds(pl.multiple_of(m * 16, 16), 16), (slice(0, 1792), slice(1792, 3456))[q]]

    c_wz = [remote(half_shard(n, q), half_shard(n, q), WZ0 + q, (flip, zmate)) for q in range(2)]
    c_wf = [
        [
            remote(half_shard(zmate, q), half_shard(zmate, q), WF0 + 3 * q + k - 1, (w, xmate(k)))
            for k in range(1, 4)
        ]
        for q in range(2)
    ]
    order = [n, xmate(1), xmate(2), xmate(3)]
    order = order + [(m + half) % nn for m in order]
    c_wc = [remote(shard(m), shard(m), WC0 + k, (w, mate)) for k, m in enumerate(order)]
    for q in range(2):
        when(late, c_wz[q].start)
    for c in c_wx:
        c.start()
    c_wc[0].start()

    loads[4].wait()
    loads[5].wait()
    for a in range(3):
        for b in range(3):
            c0 = (a * 3 + b) * 192
            w1p[b * 64:(b + 1) * 64, a * 192:(a + 1) * 192] = w1_ref[:, c0:c0 + 192]
            w2p[b * 128:(b + 1) * 128, a * 192:(a + 1) * 192] = w2_ref[c0:c0 + 192, :].T
    for d in (2, 3):
        for h in range(2, 6):
            stack1(d, h)

    def edge_rows(depths, j):
        for d in depths:
            for h in ((0, 1), (6, 7))[j]:
                stack1(d, h)

    for j in range(2):
        when(same[2 * j], c_h[1 - j].wait_recv)
    for k in range(2):
        when(jnp.logical_and(outer, d_send[k]), c_g[k].start)
    @pl.when(early)
    def _():
        pl.semaphore_wait(fsem.at[0], 1)
        for c in c_wz:
            c.start()

    edge_rows((2, 3), 0)
    when(jnp.logical_not(upper), lambda: edge_rows((2, 3), 1))
    for k in range(2):
        @pl.when(d_recv[k])
        def _():
            c_d[k].wait_recv()
            c_i[k].start()
    for d in (0, 1, 4, 5):
        for h in range(2, 6):
            stack1(d, h)
    for k in range(2):
        when(d_recv[k], c_i[k].wait_recv)
        when(jnp.logical_and(outer, d_recv[k]), c_g[k].wait_recv)
    edge_rows((0, 1, 4, 5), 0)
    when(jnp.logical_not(upper), lambda: edge_rows((0, 1, 4, 5), 1))

    def spread():
        for q in range(2):
            c_wz[q].wait_recv()
            for c in c_wf[q]:
                c.start()
        for k in range(3):
            c_wx[k].wait_recv()
        for k in range(1, 5):
            c_wc[k].start()

    def first(h0, rows):
        row = h0 * 128 + lax.broadcasted_iota(jnp.int32, (1, rows * 128), 1)
        inside = jnp.logical_and(
            jnp.logical_or(row >= 128, n > 0), jnp.logical_or(row < 640, n < nn - 1)
        )
        span = rows * 128

        def level(d, carry):
            y = jnp.dot(
                w1p[...],
                xs1[pl.ds(pl.multiple_of(d * 192, 192), 576), h0 * 128:h0 * 128 + span + 256],
                preferred_element_type=F32,
            )
            y = y[0:64, 0:span] + y[64:128, 128:span + 128] + y[128:192, 256:span + 256]
            depth = 2 * w + d - 1
            keep = jnp.logical_and(inside, jnp.logical_and(depth >= 0, depth < 2 * nw))
            y = jnp.where(keep, jnp.maximum(y, 0.0), 0.0)
            for h in range(rows):
                for e, v in enumerate(shifted(y[:, h * 128:(h + 1) * 128], 128)):
                    c0 = (h0 + h) * 128
                    xs2[pl.ds(pl.multiple_of(d * 192 + e * 64, 64), 64), c0:c0 + 128] = v
            return carry

        lax.fori_loop(0, 4, level, 0)

    def second(h0, rows):
        span = rows * 128

        def level(d):
            y = jnp.dot(
                w2p[...], xs2[d * 192:d * 192 + 576, h0 * 128:h0 * 128 + span + 256],
                preferred_element_type=F32,
            )
            return y[0:128, 0:span] + y[128:256, 128:span + 128] + y[256:384, 256:span + 256]

        s = jnp.maximum(jnp.maximum(level(0), level(1)), 0.0)
        out = []
        for r in range(rows // 2):
            t = jnp.maximum(s[:, r * 256:r * 256 + 128], s[:, r * 256 + 128:r * 256 + 256])
            out.append(jnp.maximum(t, pltpu.roll(t, 127, 1)).astype(BF))
        return out

    k_i = lax.broadcasted_iota(jnp.int32, (128, 128), 0)
    j_i = lax.broadcasted_iota(jnp.int32, (128, 128), 1)

    picks = [jnp.where(k_i == 2 * (j_i - 64 * q), 1.0, 0.0).astype(BF) for q in range(2)]

    def pack(t):
        return jnp.dot(t[0:64], picks[0], preferred_element_type=F32) + jnp.dot(
            t[64:128], picks[1], preferred_element_type=F32
        )

    @pl.when(jnp.logical_not(upper))
    def _():
        if SPREAD == 0:
            spread()
        first(0, 6)
        if SPREAD == 1:
            spread()
        r0, r1 = second(0, 4)
        keep = jnp.where(lower, 0.0, 1.0)
        pb[1, 1] = (pack(r0) * keep).astype(BF)
        pb[1, 2] = pack(r1).astype(BF)

    @pl.when(upper)
    def _():
        c_x[0].wait_recv()
        for k in range(2):
            when(d_send[k], c_x[1 + k].start)
        if SPREAD == 0:
            spread()
        for d in (2, 3):
            for h in range(6, 10):
                stack1(d, h)
        first(0, 4)
        if SPREAD == 1:
            spread()
        rb[...] = second(0, 2)[0]
        for k in range(2):
            when(d_recv[k], c_x[1 + k].wait_recv)
        for d in (0, 1, 4, 5):
            for h in range(6, 10):
                stack1(d, h)
        first(4, 4)
        r1, r2 = second(2, 4)
        pb[1, 1] = pack(rb[...]).astype(BF)
        pb[1, 2] = pack(r1).astype(BF)
        pb[1, 3] = pack(r2).astype(BF)

    def beside(i, j):
        if j == 1:
            return wok[i]
        if i == 1:
            return same[j]
        return jnp.logical_and(wok[i], same[j])

    c_e = [
        remote(pb.at[1, 1:4], pb.at[2, 1:4], E0, (w - 1, n)),
        remote(pb.at[1, 1:4], pb.at[0, 1:4], E0 + 1, (w + 1, n)),
    ]
    c_p = []
    for k, (i, j) in enumerate(near):
        src, dst = ((slice(1, 2), slice(3, 4)), (slice(1, 3), slice(1, 3)), (slice(2, 3), slice(0, 1)))[j]
        c_p.append(
            remote(pb.at[1, src], pb.at[2 - i, dst], P0 + k, (w + side(i), n + side(j)))
        )

    def plain(i, j):
        return jnp.logical_and(beside(i, j), jnp.logical_not(upper)) if j == 1 else beside(i, j)

    for k in range(2):
        when(jnp.logical_and(upper, d_send[k]), c_e[k].start)
    for k, (i, j) in enumerate(near):
        when(plain(i, j), c_p[k].start)

    if SPREAD == 2:
        spread()
    for c in c_wf[0] + c_wf[1]:
        c.wait_recv()
    for k in range(5, 8):
        c_wc[k].start()

    for k, (i, j) in enumerate(near):
        when(plain(2 - i, 2 - j), c_p[k].wait_recv)

    low = lane < 64

    @pl.when(upper)
    def _():
        for k in range(2):
            when(d_recv[k], c_e[k].wait_recv)

    def coarse_stack(first_row, taps, dst):
        def level(a, carry):
            q = [pb[a, first_row + r].astype(F32) if first_row + r < 4 else jnp.zeros((64, 128), F32) for r in range(taps + 1)]
            z = [pltpu.roll(v, 64, 1) for v in q]
            for b in range(taps):
                for c in range(2):
                    t = jnp.where(low, q[b], z[b + 1]) if c == 0 else jnp.where(low, z[b], q[b + 1])
                    for e, v in enumerate(shifted(t, 64)):
                        r0 = (b * 3 + e) * 128 + c * 64
                        dst[pl.ds(pl.multiple_of(a * taps * 384 + r0, 64), 64), :] = v
            return carry

        lax.fori_loop(0, 3, level, 0)

    coarse_stack(0, 3, xs3)
    when(upper, lambda: coarse_stack(2, 2, xs4))

    for c in c_wc:
        c.wait_recv()

    def coarse(g):
        rows = slice(g * 128, (g + 1) * 128)
        y = jnp.dot(w3g[rows, :], xs3[...], preferred_element_type=F32)

        @pl.when(lower)
        def _():
            of[rows, :] = y

        @pl.when(jnp.logical_not(lower))
        def _():
            ob[rows, :] = jnp.maximum(y, 0.0).astype(BF)

        @pl.when(upper)
        def _():
            t = None
            for a in range(3):
                p = jnp.dot(
                    w3g[rows, a * 1152:a * 1152 + 768], xs4[a * 768:(a + 1) * 768, :],
                    preferred_element_type=F32,
                )
                t = p if t is None else t + p
            of[rows, :] = t

    def block(m):
        return out_ref.at[:, pl.ds(pl.multiple_of(m * 128, 128), 128)]

    def piece(ref, m):
        return ref.at[pl.ds(pl.multiple_of(m * 16, 16), 16), :]

    def sends(m):
        return (
            remote(piece(ob, m), block(n), A0 + m, (w, m), r=A0 + n),
            remote(piece(of, m), px.at[0], B0 + m, (w, m), r=B0),
            remote(piece(of, m), px.at[1], B0 + m, (w, m), r=B0 + 1),
        )

    def drop(m):
        a, b, c = sends(m)
        when(jnp.logical_not(lower), a.wait_send)
        when(upper, b.wait_send)
        when(lower, c.wait_send)

    for g in range(2):
        coarse(g)
        if g == 0:
            @pl.when(early)
            def _():
                pl.semaphore_wait(fsem.at[1], half)
        for k in range(half):
            m = g * half + k

            @pl.when(m != n)
            def _():
                a, b, c = sends(m)
                when(jnp.logical_not(lower), a.start)
                when(upper, b.start)
                when(lower, c.start)

    @pl.when(jnp.logical_not(lower))
    def _():
        out_ref[:, pl.ds(pl.multiple_of(n * 128, 128), 128)] = ob[mine, :]

    @pl.when(upper)
    def _():
        px[0] = of[mine, :]

    @pl.when(lower)
    def _():
        px[1] = of[mine, :]

    when(same[0], c_h[0].wait_send)
    when(same[2], c_h[1].wait_send)
    for k in range(2):
        when(d_send[k], c_d[k].wait_send)
    for k in range(2):
        when(jnp.logical_and(outer, d_send[k]), c_g[k].wait_send)
        when(d_recv[k], c_i[k].wait_send)
    for k, (i, j) in enumerate(near):
        when(plain(i, j), c_p[k].wait_send)
    for c in c_wz + c_wx + c_wf[0] + c_wf[1] + c_wc:
        c.wait_send()

    @pl.when(lower)
    def _():
        c_x[0].wait_send()

    @pl.when(upper)
    def _():
        for k in range(2):
            when(d_send[k], c_x[1 + k].wait_send)
            when(d_send[k], c_e[k].wait_send)

    for m in range(nn):
        if m != half:
            when(m != n, remote(piece(ob, n), block(m), A0 + m, (w, m)).wait_recv)
    for q, home in enumerate((upper, lower)):
        when(jnp.logical_not(home), remote(piece(of, n), px.at[q], B0 + q, (w, half - 1 + q)).wait_recv)
    out_ref[:, half * 128:(half + 1) * 128] = jnp.maximum(px[0] + px[1], 0.0).astype(BF)

    for m in range(nn):
        when(m != n, functools.partial(drop, m))


def solution(mesh):
    nw, nn = mesh.shape["wide"], mesh.shape["narrow"]

    def body(stored_features, channel_scale, channel_shift, first_weight, second_weight, third_weight):
        x = stored_features.reshape(512, 128)
        out = pl.pallas_call(
            functools.partial(kernel, nw, nn),
            out_shape=pltpu.VMEM((16, nn * 128), BF),
            in_specs=[pl.BlockSpec(memory_space=pl.ANY)] * 6,
            out_specs=pl.BlockSpec(memory_space=pltpu.VMEM),
            scratch_shapes=[
                pltpu.VMEM((512, 128), BF),
                pltpu.VMEM((1, 64), F32),
                pltpu.VMEM((1, 64), F32),
                pltpu.VMEM((64, 1728), BF),
                pltpu.VMEM((1728, 128), BF),
                pltpu.VMEM((512, 128), F32),
                pltpu.VMEM((6, 64, 1280), BF),
                pltpu.VMEM((6 * 192, 1280), BF),
                pltpu.VMEM((4 * 192, 1024), BF),
                pltpu.VMEM((192, 576), BF),
                pltpu.VMEM((384, 576), BF),
                pltpu.VMEM((3, 4, 64, 128), BF),
                pltpu.VMEM((3456, 128), BF),
                pltpu.VMEM((nn * 16, 3456), BF),
                pltpu.VMEM((256, 128), BF),
                pltpu.VMEM((128, 128), BF),
                pltpu.VMEM((2304, 128), BF),
                pltpu.VMEM((256, 128), F32),
                pltpu.VMEM((2, 16, 128), F32),
                pltpu.SemaphoreType.DMA((NSEM,)),
                pltpu.SemaphoreType.DMA((NSEM,)),
                pltpu.SemaphoreType.REGULAR((2,)),
            ],
            compiler_params=pltpu.CompilerParams(collective_id=0, has_side_effects=True),
        )(x, channel_scale.reshape(1, 64), channel_shift.reshape(1, 64), first_weight, second_weight.T, third_weight)
        return out.reshape(16, 1, nn * 128)

    in_specs = (P(None, "wide", "narrow", None), P(), P(), P(), P(), P("narrow", None))
    return jax.shard_map(
        body, mesh=mesh, in_specs=in_specs, out_specs=P("narrow", "wide", None), check_vma=False
    )
```

```python
import functools

import jax
import jax.numpy as jnp
from jax import lax
from jax.experimental import pallas as pl
from jax.experimental.pallas import tpu as pltpu
from jax.sharding import PartitionSpec as P

BF = jnp.bfloat16
F32 = jnp.float32
MESH = pl.DeviceIdType.MESH

names = dict(H=2, D=2, G=4, P=8, WX=3, WZ=2, WF=6, WC=8, A=1, X=6, E=2, B=3, L=6)
BASE, NSEM = {}, 0
for name, size in names.items():
    BASE[name] = NSEM
    NSEM += size
H0, D0, G0, P0, WX0, WZ0, WF0, WC0, A0, X0, E0, B0, L0 = BASE.values()


def kernel(nw, nn, x_hbm, sc_hbm, sh_hbm, w1_hbm, w2_hbm, w3_hbm, out_ref,
           x_ref, sc_ref, sh_ref, w1_ref, w2_ref, xf, fb, xs1, xs2, w1p, w2p, pb, xs3, w3g, ob, rb, xs4, of, px, ssem, rsem, fsem):
    w = lax.axis_index("wide")
    n = lax.axis_index("narrow")
    half = nn // 2
    zh = n // half
    within = n % half
    mate = n + 1 - 2 * (n % 2)
    zmate = (n + half) % nn

    def xmate(k):
        return zh * half + (within + 2 * k) % half

    def side(i):
        return i - 1

    wok = [w > 0, None, w < nw - 1]
    nok = [n > 0, None, n < nn - 1]

    def ok(i, j):
        if i == 1:
            return nok[j]
        if j == 1:
            return wok[i]
        return jnp.logical_and(wok[i], nok[j])

    near = [(i, j) for i in range(3) for j in range(3) if (i, j) != (1, 1)]

    mine = pl.ds(pl.multiple_of(n * 16, 16), 16)
    loads = [
        pltpu.make_async_copy(src, dst, rsem.at[L0 + k])
        for k, (src, dst) in enumerate((
            (x_hbm, x_ref), (sc_hbm, sc_ref), (sh_hbm, sh_ref),
            (w3_hbm, w3g.at[mine, :]), (w1_hbm, w1_ref), (w2_hbm, w2_ref),
        ))
    ]
    loads[0].start()

    early = zh == 0
    late = zh == 1
    flip = (nw // 8 - 1 - w // 8) * 8 + w % 8 if nw % 8 == 0 else w
    cross = [jnp.logical_and(n == half, late), None, jnp.logical_and(n == half - 1, early)]
    same = [jnp.logical_and(nok[0], jnp.logical_not(cross[0])), None, jnp.logical_and(nok[2], jnp.logical_not(cross[2]))]

    def greet(sem, *dev):
        pl.semaphore_signal(sem, inc=1, device_id=dev, device_id_type=MESH)

    barrier = pltpu.get_barrier_semaphore()
    for k in range(1, half):
        greet(barrier, w, zh * half + (within + k) % half)
    for i in (0, 2):
        @pl.when(wok[i])
        def _():
            greet(barrier, w + side(i), n)
        for j in (0, 2):
            @pl.when(jnp.logical_and(wok[i], same[j]))
            def _():
                greet(barrier, w + side(i), n + side(j))

    @pl.when(early)
    def _():
        greet(barrier, flip, zmate)
        for k in range(half):
            greet(barrier, w, half + (within + k) % half)

    def count(cond):
        return jnp.where(cond, jnp.int32(1), jnp.int32(0))

    wcount = count(wok[0]) + count(wok[2])
    expected = half - 1 + wcount * (1 + count(same[0]) + count(same[2]))
    expected = expected + count(late) * (half + 1)

    for c in loads[1:]:
        c.start()

    @pl.when(jnp.logical_or(n == 0, n == half))
    def _():
        fb[:, :, 0:256] = jnp.zeros((6, 64, 256), BF)
        pb[:, 0] = jnp.zeros((3, 64, 128), BF)

    @pl.when(n == nn - 1)
    def _():
        fb[:, :, 768:1024] = jnp.zeros((6, 64, 256), BF)
        pb[:, 3] = jnp.zeros((3, 64, 128), BF)

    @pl.when(w == 0)
    def _():
        fb[0:2] = jnp.zeros((2, 64, 1280), BF)
        pb[0] = jnp.zeros((4, 64, 128), BF)

    @pl.when(w == nw - 1)
    def _():
        fb[4:6] = jnp.zeros((2, 64, 1280), BF)
        pb[2] = jnp.zeros((4, 64, 128), BF)

    lane = lax.broadcasted_iota(jnp.int32, (1, 128), 1)

    def shifted(t, period):
        pos = lane % period
        before = jnp.where(pos > 0, pltpu.roll(t, 1, 1), 0.0)
        after = jnp.where(pos < period - 1, pltpu.roll(t, 127, 1), 0.0)
        return before.astype(BF), t.astype(BF), after.astype(BF)

    def stack1(d, h):
        t = fb[d, :, h * 128:(h + 1) * 128].astype(F32)
        for e, v in enumerate(shifted(t, 128)):
            xs1[d * 192 + e * 64:d * 192 + (e + 1) * 64, h * 128:(h + 1) * 128] = v

    eye = lax.broadcasted_iota(jnp.int32, (64, 64), 0) == lax.broadcasted_iota(jnp.int32, (64, 64), 1)

    def column(ref):
        return jnp.sum(jnp.where(eye, ref[...], 0.0), axis=1, keepdims=True)

    for c in loads[:3]:
        c.wait()
    scale = column(sc_ref)
    shift = column(sh_ref)
    xf[...] = x_ref[...].astype(F32)
    for d in range(2):
        for h in range(4):
            t = xf[pl.ds(d * 4 + h, 64, stride=8), :]
            fb[2 + d, :, (2 + h) * 128:(3 + h) * 128] = (t * scale + shift).astype(BF)

    loads[3].wait()
    pl.semaphore_wait(barrier, expected)

    @pl.when(late)
    def _():
        greet(fsem.at[0], flip, zmate)
        for k in range(half):
            greet(fsem.at[1], w, (within + k) % half)

    def remote(src, dst, s, dev, r=None):
        return pltpu.make_async_remote_copy(
            src_ref=src, dst_ref=dst, send_sem=ssem.at[s], recv_sem=rsem.at[s if r is None else r],
            device_id=dev, device_id_type=MESH,
        )

    lo, hi = slice(256, 512), slice(512, 768)
    c_h = [
        remote(fb.at[2:4, :, lo], fb.at[2:4, :, 768:1024], H0, (w, n - 1)),
        remote(fb.at[2:4, :, hi], fb.at[2:4, :, 0:256], H0 + 1, (w, n + 1)),
    ]
    own = slice(256, 768)
    c_d = [
        remote(fb.at[2:4, :, own], fb.at[4:6, :, own], D0, (w - 1, n)),
        remote(fb.at[2:4, :, own], fb.at[0:2, :, own], D0 + 1, (w + 1, n)),
    ]
    d_send = [wok[0], wok[2]]
    d_recv = [wok[2], wok[0]]
    even = n % 2 == 0
    outer = jnp.logical_or(jnp.logical_and(even, same[0]), jnp.logical_and(jnp.logical_not(even), same[2]))

    def rows_at(on_even, on_odd):
        return pl.ds(pl.multiple_of(jnp.where(even, on_even, on_odd), 256), 256)

    outside = rows_at(0, 768)
    c_g = [
        remote(fb.at[2:4, :, outside], fb.at[4:6, :, outside], G0, (w - 1, n)),
        remote(fb.at[2:4, :, outside], fb.at[0:2, :, outside], G0 + 1, (w + 1, n)),
    ]
    depths = (slice(4, 6), slice(0, 2))
    c_i = [
        remote(fb.at[depths[k], :, rows_at(512, 256)], fb.at[depths[k], :, rows_at(0, 768)], G0 + 2 + k, (w, mate))
        for k in range(2)
    ]
    far = slice(768, 1280)
    c_x = [
        [
            remote(fb.at[2 + i:3 + i, :, own], fb.at[2 + i:3 + i, :, far], X0 + i, (w, n - 1)),
            remote(fb.at[2 + i:3 + i, :, far], fb.at[4 + i:5 + i, :, far], X0 + 2 + i, (w - 1, n)),
            remote(fb.at[2 + i:3 + i, :, far], fb.at[i:1 + i, :, far], X0 + 4 + i, (w + 1, n)),
        ]
        for i in range(2)
    ]

    def when(cond, f):
        pl.when(cond)(f)

    upper = cross[2]
    lower = cross[0]
    for i in range(2):
        when(lower, c_x[i][0].start)
    when(same[0], c_h[0].start)
    when(same[2], c_h[1].start)
    for k in range(2):
        when(d_send[k], c_d[k].start)

    def shard(m):
        return w3g.at[pl.ds(pl.multiple_of(m * 16, 16), 16), :]

    c_wx = [remote(shard(n), shard(n), WX0 + k - 1, (w, xmate(k))) for k in range(1, 4)]

    def half_shard(m, q):
        return w3g.at[pl.ds(pl.multiple_of(m * 16, 16), 16), (slice(0, 1792), slice(1792, 3456))[q]]

    c_wz = [remote(half_shard(n, q), half_shard(n, q), WZ0 + q, (flip, zmate)) for q in range(2)]
    c_wf = [
        [
            remote(half_shard(zmate, q), half_shard(zmate, q), WF0 + 3 * q + k - 1, (w, xmate(k)))
            for k in range(1, 4)
        ]
        for q in range(2)
    ]
    order = [n, xmate(1), xmate(2), xmate(3)]
    order = order + [(m + half) % nn for m in order]
    c_wc = [remote(shard(m), shard(m), WC0 + k, (w, mate)) for k, m in enumerate(order)]
    for q in range(2):
        when(late, c_wz[q].start)
    for c in c_wx:
        c.start()
    c_wc[0].start()

    loads[4].wait()
    loads[5].wait()
    for a in range(3):
        for b in range(3):
            c0 = (a * 3 + b) * 192
            w1p[b * 64:(b + 1) * 64, a * 192:(a + 1) * 192] = w1_ref[:, c0:c0 + 192]
            w2p[b * 128:(b + 1) * 128, a * 192:(a + 1) * 192] = w2_ref[c0:c0 + 192, :].T
    for d in (2, 3):
        for h in range(2, 6):
            stack1(d, h)

    def edge_rows(depths, j):
        for d in depths:
            for h in ((0, 1), (6, 7))[j]:
                stack1(d, h)

    for j in range(2):
        when(same[2 * j], c_h[1 - j].wait_recv)
    for k in range(2):
        when(jnp.logical_and(outer, d_send[k]), c_g[k].start)
    @pl.when(early)
    def _():
        pl.semaphore_wait(fsem.at[0], 1)
        for c in c_wz:
            c.start()

    edge_rows((2, 3), 0)
    when(jnp.logical_not(upper), lambda: edge_rows((2, 3), 1))
    for k in range(2):
        @pl.when(d_recv[k])
        def _():
            c_d[k].wait_recv()
            c_i[k].start()
    for d in (0, 1, 4, 5):
        for h in range(2, 6):
            stack1(d, h)
    for k in range(2):
        when(d_recv[k], c_i[k].wait_recv)
        when(jnp.logical_and(outer, d_recv[k]), c_g[k].wait_recv)
    edge_rows((0, 1, 4, 5), 0)
    when(jnp.logical_not(upper), lambda: edge_rows((0, 1, 4, 5), 1))

    def spread():
        for q in range(2):
            c_wz[q].wait_recv()
            for c in c_wf[q]:
                c.start()
        for k in range(3):
            c_wx[k].wait_recv()
        for k in range(1, 5):
            c_wc[k].start()

    def first(h0, rows):
        row = h0 * 128 + lax.broadcasted_iota(jnp.int32, (1, rows * 128), 1)
        inside = jnp.logical_and(
            jnp.logical_or(row >= 128, n > 0), jnp.logical_or(row < 640, n < nn - 1)
        )
        span = rows * 128

        def level(d, carry):
            y = jnp.dot(
                w1p[...],
                xs1[pl.ds(pl.multiple_of(d * 192, 192), 576), h0 * 128:h0 * 128 + span + 256],
                preferred_element_type=F32,
            )
            y = y[0:64, 0:span] + y[64:128, 128:span + 128] + y[128:192, 256:span + 256]
            depth = 2 * w + d - 1
            keep = jnp.logical_and(inside, jnp.logical_and(depth >= 0, depth < 2 * nw))
            y = jnp.where(keep, jnp.maximum(y, 0.0), 0.0)
            for h in range(rows):
                for e, v in enumerate(shifted(y[:, h * 128:(h + 1) * 128], 128)):
                    c0 = (h0 + h) * 128
                    xs2[pl.ds(pl.multiple_of(d * 192 + e * 64, 64), 64), c0:c0 + 128] = v
            return carry

        lax.fori_loop(0, 4, level, 0)

    def second(h0, rows):
        span = rows * 128

        def level(d):
            y = jnp.dot(
                w2p[...], xs2[d * 192:d * 192 + 576, h0 * 128:h0 * 128 + span + 256],
                preferred_element_type=F32,
            )
            return y[0:128, 0:span] + y[128:256, 128:span + 128] + y[256:384, 256:span + 256]

        s = jnp.maximum(jnp.maximum(level(0), level(1)), 0.0)
        out = []
        for r in range(rows // 2):
            t = jnp.maximum(s[:, r * 256:r * 256 + 128], s[:, r * 256 + 128:r * 256 + 256])
            out.append(jnp.maximum(t, pltpu.roll(t, 127, 1)).astype(BF))
        return out

    k_i = lax.broadcasted_iota(jnp.int32, (128, 128), 0)
    j_i = lax.broadcasted_iota(jnp.int32, (128, 128), 1)

    picks = [jnp.where(k_i == 2 * (j_i - 64 * q), 1.0, 0.0).astype(BF) for q in range(2)]

    def pack(t):
        return jnp.dot(t[0:64], picks[0], preferred_element_type=F32) + jnp.dot(
            t[64:128], picks[1], preferred_element_type=F32
        )

    @pl.when(jnp.logical_not(upper))
    def _():
        when(late, spread)
        first(0, 6)
        r0, r1 = second(0, 4)
        keep = jnp.where(lower, 0.0, 1.0)
        pb[1, 1] = (pack(r0) * keep).astype(BF)
        pb[1, 2] = pack(r1).astype(BF)

    @pl.when(upper)
    def _():
        for i in range(2):
            c_x[i][0].wait_recv()
            for k in range(2):
                when(d_send[k], c_x[i][1 + k].start)
        for d in (2, 3):
            for h in range(6, 10):
                stack1(d, h)
        first(0, 4)
        rb[...] = second(0, 2)[0]
        for k in range(2):
            for i in range(2):
                when(d_recv[k], c_x[i][1 + k].wait_recv)
        for d in (0, 1, 4, 5):
            for h in range(6, 10):
                stack1(d, h)
        first(4, 4)
        r1, r2 = second(2, 4)
        pb[1, 1] = pack(rb[...]).astype(BF)
        pb[1, 2] = pack(r1).astype(BF)
        pb[1, 3] = pack(r2).astype(BF)

    def beside(i, j):
        if j == 1:
            return wok[i]
        if i == 1:
            return same[j]
        return jnp.logical_and(wok[i], same[j])

    c_e = [
        remote(pb.at[1, 1:4], pb.at[2, 1:4], E0, (w - 1, n)),
        remote(pb.at[1, 1:4], pb.at[0, 1:4], E0 + 1, (w + 1, n)),
    ]
    c_p = []
    for k, (i, j) in enumerate(near):
        src, dst = ((slice(1, 2), slice(3, 4)), (slice(1, 3), slice(1, 3)), (slice(2, 3), slice(0, 1)))[j]
        c_p.append(
            remote(pb.at[1, src], pb.at[2 - i, dst], P0 + k, (w + side(i), n + side(j)))
        )

    def plain(i, j):
        return jnp.logical_and(beside(i, j), jnp.logical_not(upper)) if j == 1 else beside(i, j)

    for k in range(2):
        when(jnp.logical_and(upper, d_send[k]), c_e[k].start)
    for k, (i, j) in enumerate(near):
        when(plain(i, j), c_p[k].start)

    def spread_rest():
        for k in range(3):
            for q in range(2):
                c_wf[q][k].wait_recv()
            c_wc[7 - k].start()

    when(early, spread)
    when(late, spread_rest)
    for k, (i, j) in enumerate(near):
        when(plain(2 - i, 2 - j), c_p[k].wait_recv)

    low = lane < 64

    @pl.when(upper)
    def _():
        for k in range(2):
            when(d_recv[k], c_e[k].wait_recv)

    def coarse_stack(first_row, taps, dst):
        def level(a, carry):
            q = [pb[a, first_row + r].astype(F32) if first_row + r < 4 else jnp.zeros((64, 128), F32) for r in range(taps + 1)]
            z = [pltpu.roll(v, 64, 1) for v in q]
            for b in range(taps):
                for c in range(2):
                    t = jnp.where(low, q[b], z[b + 1]) if c == 0 else jnp.where(low, z[b], q[b + 1])
                    for e, v in enumerate(shifted(t, 64)):
                        r0 = (b * 3 + e) * 128 + c * 64
                        dst[pl.ds(pl.multiple_of(a * taps * 384 + r0, 64), 64), :] = v
            return carry

        lax.fori_loop(0, 3, level, 0)

    coarse_stack(0, 3, xs3)
    when(upper, lambda: coarse_stack(2, 2, xs4))

    for c in c_wc[:4]:
        c.wait_recv()

    @pl.when(late)
    def _():
        for c in c_wc[4:]:
            c.wait_recv()

    def coarse(g):
        rows = slice(g * 128, (g + 1) * 128)
        y = jnp.dot(w3g[rows, :], xs3[...], preferred_element_type=F32)

        @pl.when(lower)
        def _():
            of[rows, :] = y

        @pl.when(jnp.logical_not(lower))
        def _():
            ob[rows, :] = jnp.maximum(y, 0.0).astype(BF)

        @pl.when(upper)
        def _():
            t = None
            for a in range(3):
                p = jnp.dot(
                    w3g[rows, a * 1152:a * 1152 + 768], xs4[a * 768:(a + 1) * 768, :],
                    preferred_element_type=F32,
                )
                t = p if t is None else t + p
            of[rows, :] = t

    def block(m):
        return out_ref.at[:, pl.ds(pl.multiple_of(m * 128, 128), 128)]

    def piece(ref, m):
        return ref.at[pl.ds(pl.multiple_of(m * 16, 16), 16), :]

    def sends(m):
        return (
            remote(piece(ob, m), block(n), A0, (w, m)),
            remote(piece(of, m), px.at[0], B0 + 2, (w, m), r=B0),
            remote(piece(of, m), px.at[1], B0 + 2, (w, m), r=B0 + 1),
        )

    for g in range(2):
        if g == 1:
            @pl.when(early)
            def _():
                spread_rest()
                for c in c_wc[4:]:
                    c.wait_recv()
                pl.semaphore_wait(fsem.at[1], half)
        coarse(g)
        group = range(g * half, (g + 1) * half)

        @pl.when(jnp.logical_not(lower))
        def _():
            for m in group:
                when(m != n, sends(m)[0].start)

        for q, home in enumerate((upper, lower)):
            @pl.when(home)
            def _():
                for m in group:
                    if m != half - 1 + q:
                        sends(m)[1 + q].start()

    @pl.when(jnp.logical_not(lower))
    def _():
        out_ref[:, pl.ds(pl.multiple_of(n * 128, 128), 128)] = ob[mine, :]

    @pl.when(upper)
    def _():
        px[0] = of[mine, :]

    @pl.when(lower)
    def _():
        px[1] = of[mine, :]

    when(same[0], c_h[0].wait_send)
    when(same[2], c_h[1].wait_send)
    for k in range(2):
        when(d_send[k], c_d[k].wait_send)
    for k in range(2):
        when(jnp.logical_and(outer, d_send[k]), c_g[k].wait_send)
        when(d_recv[k], c_i[k].wait_send)
    for k, (i, j) in enumerate(near):
        when(plain(i, j), c_p[k].wait_send)
    for c in c_wz + c_wx + c_wf[0] + c_wf[1] + c_wc:
        c.wait_send()

    @pl.when(lower)
    def _():
        for i in range(2):
            c_x[i][0].wait_send()

    @pl.when(upper)
    def _():
        for k in range(2):
            for i in range(2):
                when(d_send[k], c_x[i][1 + k].wait_send)
            when(d_send[k], c_e[k].wait_send)

    def many(count):
        return remote(ob.at[0:16 * count, :], ob.at[0:16 * count, :], A0, (w, mate))

    when(lower, many(nn - 1).wait_recv)
    when(jnp.logical_not(lower), many(nn - 2).wait_recv)
    for q, home in enumerate((upper, lower)):
        when(jnp.logical_not(home), remote(piece(of, n), px.at[q], B0 + q, (w, half - 1 + q)).wait_recv)
    out_ref[:, half * 128:(half + 1) * 128] = jnp.maximum(px[0] + px[1], 0.0).astype(BF)

    when(jnp.logical_not(lower), many(nn - 1).wait_send)
    parts = of.at[0:16 * (nn - 1), :]
    when(jnp.logical_or(upper, lower), remote(parts, parts, B0 + 2, (w, mate)).wait_send)


def solution(mesh):
    nw, nn = mesh.shape["wide"], mesh.shape["narrow"]

    def body(stored_features, channel_scale, channel_shift, first_weight, second_weight, third_weight):
        x = stored_features.reshape(512, 128)
        out = pl.pallas_call(
            functools.partial(kernel, nw, nn),
            out_shape=pltpu.VMEM((16, nn * 128), BF),
            in_specs=[pl.BlockSpec(memory_space=pl.ANY)] * 6,
            out_specs=pl.BlockSpec(memory_space=pltpu.VMEM),
            scratch_shapes=[
                pltpu.VMEM((512, 128), BF),
                pltpu.VMEM((1, 64), F32),
                pltpu.VMEM((1, 64), F32),
                pltpu.VMEM((64, 1728), BF),
                pltpu.VMEM((1728, 128), BF),
                pltpu.VMEM((512, 128), F32),
                pltpu.VMEM((6, 64, 1280), BF),
                pltpu.VMEM((6 * 192, 1280), BF),
                pltpu.VMEM((4 * 192, 1024), BF),
                pltpu.VMEM((192, 576), BF),
                pltpu.VMEM((384, 576), BF),
                pltpu.VMEM((3, 4, 64, 128), BF),
                pltpu.VMEM((3456, 128), BF),
                pltpu.VMEM((nn * 16, 3456), BF),
                pltpu.VMEM((256, 128), BF),
                pltpu.VMEM((128, 128), BF),
                pltpu.VMEM((2304, 128), BF),
                pltpu.VMEM((256, 128), F32),
                pltpu.VMEM((2, 16, 128), F32),
                pltpu.SemaphoreType.DMA((NSEM,)),
                pltpu.SemaphoreType.DMA((NSEM,)),
                pltpu.SemaphoreType.REGULAR((2,)),
            ],
            compiler_params=pltpu.CompilerParams(collective_id=0, has_side_effects=True),
        )(x, channel_scale.reshape(1, 64), channel_shift.reshape(1, 64), first_weight, second_weight.T, third_weight)
        return out.reshape(16, 1, nn * 128)

    in_specs = (P(None, "wide", "narrow", None), P(), P(), P(), P(), P("narrow", None))
    return jax.shard_map(
        body, mesh=mesh, in_specs=in_specs, out_specs=P("narrow", "wide", None), check_vma=False
    )
```

```python
import functools

import jax
import jax.numpy as jnp
from jax import lax
from jax.experimental import pallas as pl
from jax.experimental.pallas import tpu as pltpu
from jax.sharding import PartitionSpec as P

BF = jnp.bfloat16
F32 = jnp.float32
MESH = pl.DeviceIdType.MESH

names = dict(H=2, D=2, G=4, P=8, WX=3, WZ=2, WF=6, WC=8, A=1, X=6, E=2, B=3, L=6)
BASE, NSEM = {}, 0
for name, size in names.items():
    BASE[name] = NSEM
    NSEM += size
H0, D0, G0, P0, WX0, WZ0, WF0, WC0, A0, X0, E0, B0, L0 = BASE.values()


def kernel(nw, nn, x_hbm, sc_hbm, sh_hbm, w1_hbm, w2_hbm, w3_hbm, out_ref,
           x_ref, sc_ref, sh_ref, w1_ref, w2_ref, xf, fb, xs1, xs2, w1p, w2p, pb, xs3, w3g, ob, rb, of, px, ssem, rsem, fsem):
    w = lax.axis_index("wide")
    n = lax.axis_index("narrow")
    half = nn // 2
    zh = n // half
    within = n % half
    mate = n + 1 - 2 * (n % 2)
    zmate = (n + half) % nn

    def xmate(k):
        return zh * half + (within + 2 * k) % half

    def side(i):
        return i - 1

    wok = [w > 0, None, w < nw - 1]
    nok = [n > 0, None, n < nn - 1]

    def ok(i, j):
        if i == 1:
            return nok[j]
        if j == 1:
            return wok[i]
        return jnp.logical_and(wok[i], nok[j])

    near = [(i, j) for i in range(3) for j in range(3) if (i, j) != (1, 1)]

    mine = pl.ds(pl.multiple_of(n * 16, 16), 16)
    loads = [
        pltpu.make_async_copy(src, dst, rsem.at[L0 + k])
        for k, (src, dst) in enumerate((
            (x_hbm, x_ref), (sc_hbm, sc_ref), (sh_hbm, sh_ref),
            (w3_hbm, w3g.at[mine, :]), (w1_hbm, w1_ref), (w2_hbm, w2_ref),
        ))
    ]
    loads[0].start()

    early = zh == 0
    late = zh == 1
    flip = (nw // 8 - 1 - w // 8) * 8 + w % 8 if nw % 8 == 0 else w
    cross = [jnp.logical_and(n == half, late), None, jnp.logical_and(n == half - 1, early)]
    same = [jnp.logical_and(nok[0], jnp.logical_not(cross[0])), None, jnp.logical_and(nok[2], jnp.logical_not(cross[2]))]

    def greet(sem, *dev):
        pl.semaphore_signal(sem, inc=1, device_id=dev, device_id_type=MESH)

    barrier = pltpu.get_barrier_semaphore()
    for k in range(1, half):
        greet(barrier, w, zh * half + (within + k) % half)
    for i in (0, 2):
        @pl.when(wok[i])
        def _():
            greet(barrier, w + side(i), n)
        for j in (0, 2):
            @pl.when(jnp.logical_and(wok[i], same[j]))
            def _():
                greet(barrier, w + side(i), n + side(j))

    @pl.when(early)
    def _():
        greet(barrier, flip, zmate)
        for k in range(half):
            greet(barrier, w, half + (within + k) % half)

    def count(cond):
        return jnp.where(cond, jnp.int32(1), jnp.int32(0))

    wcount = count(wok[0]) + count(wok[2])
    expected = half - 1 + wcount * (1 + count(same[0]) + count(same[2]))
    expected = expected + count(late) * (half + 1)

    for c in loads[1:]:
        c.start()

    @pl.when(jnp.logical_or(n == 0, n == half))
    def _():
        fb[:, :, 0:256] = jnp.zeros((6, 64, 256), BF)
        pb[:, 0] = jnp.zeros((3, 64, 128), BF)

    @pl.when(n == nn - 1)
    def _():
        fb[:, :, 768:1024] = jnp.zeros((6, 64, 256), BF)
        pb[:, 3] = jnp.zeros((3, 64, 128), BF)

    @pl.when(w == 0)
    def _():
        fb[0:2] = jnp.zeros((2, 64, 1280), BF)
        pb[0] = jnp.zeros((4, 64, 128), BF)

    @pl.when(w == nw - 1)
    def _():
        fb[4:6] = jnp.zeros((2, 64, 1280), BF)
        pb[2] = jnp.zeros((4, 64, 128), BF)

    lane = lax.broadcasted_iota(jnp.int32, (1, 128), 1)

    def shifted(t, period):
        pos = lane % period
        before = jnp.where(pos > 0, pltpu.roll(t, 1, 1), 0.0)
        after = jnp.where(pos < period - 1, pltpu.roll(t, 127, 1), 0.0)
        return before.astype(BF), t.astype(BF), after.astype(BF)

    def stack1(d, h):
        t = fb[d, :, h * 128:(h + 1) * 128].astype(F32)
        for e, v in enumerate(shifted(t, 128)):
            xs1[d * 192 + e * 64:d * 192 + (e + 1) * 64, h * 128:(h + 1) * 128] = v

    eye = lax.broadcasted_iota(jnp.int32, (64, 64), 0) == lax.broadcasted_iota(jnp.int32, (64, 64), 1)

    def column(ref):
        return jnp.sum(jnp.where(eye, ref[...], 0.0), axis=1, keepdims=True)

    for c in loads[:3]:
        c.wait()
    scale = column(sc_ref)
    shift = column(sh_ref)
    xf[...] = x_ref[...].astype(F32)
    for d in range(2):
        for h in range(4):
            t = xf[pl.ds(d * 4 + h, 64, stride=8), :]
            fb[2 + d, :, (2 + h) * 128:(3 + h) * 128] = (t * scale + shift).astype(BF)

    loads[3].wait()
    pl.semaphore_wait(barrier, expected)

    @pl.when(late)
    def _():
        greet(fsem.at[0], flip, zmate)
        for k in range(half):
            greet(fsem.at[1], w, (within + k) % half)

    def remote(src, dst, s, dev, r=None):
        return pltpu.make_async_remote_copy(
            src_ref=src, dst_ref=dst, send_sem=ssem.at[s], recv_sem=rsem.at[s if r is None else r],
            device_id=dev, device_id_type=MESH,
        )

    lo, hi = slice(256, 512), slice(512, 768)
    c_h = [
        remote(fb.at[2:4, :, lo], fb.at[2:4, :, 768:1024], H0, (w, n - 1)),
        remote(fb.at[2:4, :, hi], fb.at[2:4, :, 0:256], H0 + 1, (w, n + 1)),
    ]
    own = slice(256, 768)
    c_d = [
        remote(fb.at[2:4, :, own], fb.at[4:6, :, own], D0, (w - 1, n)),
        remote(fb.at[2:4, :, own], fb.at[0:2, :, own], D0 + 1, (w + 1, n)),
    ]
    d_send = [wok[0], wok[2]]
    d_recv = [wok[2], wok[0]]
    even = n % 2 == 0
    outer = jnp.logical_or(jnp.logical_and(even, same[0]), jnp.logical_and(jnp.logical_not(even), same[2]))

    def rows_at(on_even, on_odd):
        return pl.ds(pl.multiple_of(jnp.where(even, on_even, on_odd), 256), 256)

    outside = rows_at(0, 768)
    c_g = [
        remote(fb.at[2:4, :, outside], fb.at[4:6, :, outside], G0, (w - 1, n)),
        remote(fb.at[2:4, :, outside], fb.at[0:2, :, outside], G0 + 1, (w + 1, n)),
    ]
    depths = (slice(4, 6), slice(0, 2))
    c_i = [
        remote(fb.at[depths[k], :, rows_at(512, 256)], fb.at[depths[k], :, rows_at(0, 768)], G0 + 2 + k, (w, mate))
        for k in range(2)
    ]
    far = slice(768, 1280)
    c_x = [
        [
            remote(fb.at[2 + i:3 + i, :, own], fb.at[2 + i:3 + i, :, far], X0 + i, (w, n - 1)),
            remote(fb.at[2 + i:3 + i, :, far], fb.at[4 + i:5 + i, :, far], X0 + 2 + i, (w - 1, n)),
            remote(fb.at[2 + i:3 + i, :, far], fb.at[i:1 + i, :, far], X0 + 4 + i, (w + 1, n)),
        ]
        for i in range(2)
    ]

    def when(cond, f):
        pl.when(cond)(f)

    upper = cross[2]
    lower = cross[0]
    for i in range(2):
        when(lower, c_x[i][0].start)
    when(same[0], c_h[0].start)
    when(same[2], c_h[1].start)
    near_cut = n == half + 1
    held = [jnp.logical_and(near_cut, w == nw // 4), jnp.logical_and(near_cut, w == 3 * nw // 4 - 1)]
    for k in range(2):
        when(jnp.logical_and(d_send[k], jnp.logical_not(held[k])), c_d[k].start)

    def shard(m):
        return w3g.at[pl.ds(pl.multiple_of(m * 16, 16), 16), :]

    c_wx = [remote(shard(n), shard(n), WX0 + k - 1, (w, xmate(k))) for k in range(1, 4)]

    def half_shard(m, q):
        return w3g.at[pl.ds(pl.multiple_of(m * 16, 16), 16), (slice(0, 1792), slice(1792, 3456))[q]]

    c_wz = [remote(half_shard(n, q), half_shard(n, q), WZ0 + q, (flip, zmate)) for q in range(2)]
    c_wf = [
        [
            remote(half_shard(zmate, q), half_shard(zmate, q), WF0 + 3 * q + k - 1, (w, xmate(k)))
            for k in range(1, 4)
        ]
        for q in range(2)
    ]
    order = [n, xmate(1), xmate(2), xmate(3)]
    order = order + [(m + half) % nn for m in order]
    c_wc = [remote(shard(m), shard(m), WC0 + k, (w, mate)) for k, m in enumerate(order)]
    for q in range(2):
        when(late, c_wz[q].start)
    for c in c_wx:
        c.start()
    c_wc[0].start()

    loads[4].wait()
    loads[5].wait()
    for a in range(3):
        for b in range(3):
            c0 = (a * 3 + b) * 192
            w1p[b * 64:(b + 1) * 64, a * 192:(a + 1) * 192] = w1_ref[:, c0:c0 + 192]
            w2p[b * 128:(b + 1) * 128, a * 192:(a + 1) * 192] = w2_ref[c0:c0 + 192, :].T
    for d in (2, 3):
        for h in range(2, 6):
            stack1(d, h)

    def edge_rows(depths, j):
        for d in depths:
            for h in ((0, 1), (6, 7))[j]:
                stack1(d, h)

    for j in range(2):
        when(same[2 * j], c_h[1 - j].wait_recv)
    for k in range(2):
        when(jnp.logical_and(d_send[k], held[k]), c_d[k].start)
    for k in range(2):
        when(jnp.logical_and(outer, d_send[k]), c_g[k].start)
    @pl.when(early)
    def _():
        pl.semaphore_wait(fsem.at[0], 1)
        for c in c_wz:
            c.start()

    edge_rows((2, 3), 0)
    when(jnp.logical_not(upper), lambda: edge_rows((2, 3), 1))
    for k in range(2):
        @pl.when(d_recv[k])
        def _():
            c_d[k].wait_recv()
            c_i[k].start()
    for d in (0, 1, 4, 5):
        for h in range(2, 6):
            stack1(d, h)
    for k in range(2):
        when(d_recv[k], c_i[k].wait_recv)
        when(jnp.logical_and(outer, d_recv[k]), c_g[k].wait_recv)
    edge_rows((0, 1, 4, 5), 0)
    when(jnp.logical_not(upper), lambda: edge_rows((0, 1, 4, 5), 1))

    def spread():
        for q in range(2):
            c_wz[q].wait_recv()
            for c in c_wf[q]:
                c.start()
        for k in range(3):
            c_wx[k].wait_recv()
        for k in range(1, 5):
            c_wc[k].start()

    def first(h0, rows):
        row = h0 * 128 + lax.broadcasted_iota(jnp.int32, (1, rows * 128), 1)
        inside = jnp.logical_and(
            jnp.logical_or(row >= 128, n > 0), jnp.logical_or(row < 640, n < nn - 1)
        )
        span = rows * 128

        def level(d, carry):
            y = jnp.dot(
                w1p[...],
                xs1[pl.ds(pl.multiple_of(d * 192, 192), 576), h0 * 128:h0 * 128 + span + 256],
                preferred_element_type=F32,
            )
            y = y[0:64, 0:span] + y[64:128, 128:span + 128] + y[128:192, 256:span + 256]
            depth = 2 * w + d - 1
            keep = jnp.logical_and(inside, jnp.logical_and(depth >= 0, depth < 2 * nw))
            y = jnp.where(keep, jnp.maximum(y, 0.0), 0.0)
            for h in range(rows):
                for e, v in enumerate(shifted(y[:, h * 128:(h + 1) * 128], 128)):
                    c0 = (h0 + h) * 128
                    xs2[pl.ds(pl.multiple_of(d * 192 + e * 64, 64), 64), c0:c0 + 128] = v
            return carry

        lax.fori_loop(0, 4, level, 0)

    def second(h0, rows):
        span = rows * 128

        def level(d):
            y = jnp.dot(
                w2p[...], xs2[d * 192:d * 192 + 576, h0 * 128:h0 * 128 + span + 256],
                preferred_element_type=F32,
            )
            return y[0:128, 0:span] + y[128:256, 128:span + 128] + y[256:384, 256:span + 256]

        s = jnp.maximum(jnp.maximum(level(0), level(1)), 0.0)
        out = []
        for r in range(rows // 2):
            t = jnp.maximum(s[:, r * 256:r * 256 + 128], s[:, r * 256 + 128:r * 256 + 256])
            out.append(jnp.maximum(t, pltpu.roll(t, 127, 1)).astype(BF))
        return out

    k_i = lax.broadcasted_iota(jnp.int32, (128, 128), 0)
    j_i = lax.broadcasted_iota(jnp.int32, (128, 128), 1)

    picks = [jnp.where(k_i == 2 * (j_i - 64 * q), 1.0, 0.0).astype(BF) for q in range(2)]

    def pack(t):
        return jnp.dot(t[0:64], picks[0], preferred_element_type=F32) + jnp.dot(
            t[64:128], picks[1], preferred_element_type=F32
        )

    @pl.when(jnp.logical_not(upper))
    def _():
        when(late, spread)
        first(0, 6)
        r0, r1 = second(0, 4)
        keep = jnp.where(lower, 0.0, 1.0)
        pb[1, 1] = (pack(r0) * keep).astype(BF)
        pb[1, 2] = pack(r1).astype(BF)

    @pl.when(upper)
    def _():
        for a in range(3):
            xs3[a * 1152 + 768:(a + 1) * 1152, 128:256] = jnp.zeros((384, 128), BF)
        for i in range(2):
            c_x[i][0].wait_recv()
            for k in range(2):
                when(d_send[k], c_x[i][1 + k].start)
        for d in (2, 3):
            for h in range(6, 10):
                stack1(d, h)
        first(0, 4)
        rb[...] = second(0, 2)[0]
        spread()
        for k in range(2):
            for i in range(2):
                when(d_recv[k], c_x[i][1 + k].wait_recv)
        for d in (0, 1, 4, 5):
            for h in range(6, 10):
                stack1(d, h)
        first(4, 4)
        r1, r2 = second(2, 4)
        pb[1, 1] = pack(rb[...]).astype(BF)
        pb[1, 2] = pack(r1).astype(BF)
        pb[1, 3] = pack(r2).astype(BF)

    def beside(i, j):
        if j == 1:
            return wok[i]
        if i == 1:
            return same[j]
        return jnp.logical_and(wok[i], same[j])

    c_e = [
        remote(pb.at[1, 1:4], pb.at[2, 1:4], E0, (w - 1, n)),
        remote(pb.at[1, 1:4], pb.at[0, 1:4], E0 + 1, (w + 1, n)),
    ]
    c_p = []
    for k, (i, j) in enumerate(near):
        src, dst = ((slice(1, 2), slice(3, 4)), (slice(1, 3), slice(1, 3)), (slice(2, 3), slice(0, 1)))[j]
        c_p.append(
            remote(pb.at[1, src], pb.at[2 - i, dst], P0 + k, (w + side(i), n + side(j)))
        )

    def plain(i, j):
        return jnp.logical_and(beside(i, j), jnp.logical_not(upper)) if j == 1 else beside(i, j)

    for k in range(2):
        when(jnp.logical_and(upper, d_send[k]), c_e[k].start)
    for k, (i, j) in enumerate(near):
        when(plain(i, j), c_p[k].start)

    def spread_rest():
        for k in range(3):
            for q in range(2):
                c_wf[q][k].wait_recv()
            c_wc[7 - k].start()

    when(jnp.logical_and(early, jnp.logical_not(upper)), spread)
    when(late, spread_rest)
    for k, (i, j) in enumerate(near):
        when(plain(2 - i, 2 - j), c_p[k].wait_recv)

    low = lane < 64

    @pl.when(upper)
    def _():
        for k in range(2):
            when(d_recv[k], c_e[k].wait_recv)

    def coarse_stack(first_row, taps, dst, cols):
        def level(a, carry):
            q = [pb[a, first_row + r].astype(F32) if first_row + r < 4 else jnp.zeros((64, 128), F32) for r in range(taps + 1)]
            z = [pltpu.roll(v, 64, 1) for v in q]
            for b in range(taps):
                for c in range(2):
                    t = jnp.where(low, q[b], z[b + 1]) if c == 0 else jnp.where(low, z[b], q[b + 1])
                    for e, v in enumerate(shifted(t, 64)):
                        r0 = (b * 3 + e) * 128 + c * 64
                        dst[pl.ds(pl.multiple_of(a * 1152 + r0, 64), 64), cols] = v
            return carry

        lax.fori_loop(0, 3, level, 0)

    coarse_stack(0, 3, xs3, slice(0, 128))
    when(upper, lambda: coarse_stack(2, 2, xs3, slice(128, 256)))

    for c in c_wc[:4]:
        c.wait_recv()

    @pl.when(late)
    def _():
        for c in c_wc[4:]:
            c.wait_recv()

    def coarse(g):
        rows = slice(g * 128, (g + 1) * 128)

        @pl.when(jnp.logical_not(upper))
        def _():
            y = jnp.dot(w3g[rows, :], xs3[:, 0:128], preferred_element_type=F32)

            @pl.when(lower)
            def _():
                of[rows, :] = y

            @pl.when(jnp.logical_not(lower))
            def _():
                ob[rows, :] = jnp.maximum(y, 0.0).astype(BF)

        @pl.when(upper)
        def _():
            y = jnp.dot(w3g[rows, :], xs3[...], preferred_element_type=F32)
            ob[rows, :] = jnp.maximum(y[:, 0:128], 0.0).astype(BF)
            of[rows, :] = y[:, 128:256]

    def block(m):
        return out_ref.at[:, pl.ds(pl.multiple_of(m * 128, 128), 128)]

    def piece(ref, m):
        return ref.at[pl.ds(pl.multiple_of(m * 16, 16), 16), :]

    def sends(m):
        return (
            remote(piece(ob, m), block(n), A0, (w, m)),
            remote(piece(of, m), px.at[0], B0 + 2, (w, m), r=B0),
            remote(piece(of, m), px.at[1], B0 + 2, (w, m), r=B0 + 1),
        )

    for g in range(2):
        if g == 1:
            @pl.when(early)
            def _():
                spread_rest()
                for c in c_wc[4:]:
                    c.wait_recv()
                pl.semaphore_wait(fsem.at[1], half)
        coarse(g)
        group = range(g * half, (g + 1) * half)

        @pl.when(jnp.logical_not(lower))
        def _():
            for m in group:
                when(m != n, sends(m)[0].start)

        for q, home in enumerate((upper, lower)):
            @pl.when(home)
            def _():
                for m in group:
                    if m != half - 1 + q:
                        sends(m)[1 + q].start()

    @pl.when(jnp.logical_not(lower))
    def _():
        out_ref[:, pl.ds(pl.multiple_of(n * 128, 128), 128)] = ob[mine, :]

    @pl.when(upper)
    def _():
        px[0] = of[mine, :]

    @pl.when(lower)
    def _():
        px[1] = of[mine, :]

    when(same[0], c_h[0].wait_send)
    when(same[2], c_h[1].wait_send)
    for k in range(2):
        when(d_send[k], c_d[k].wait_send)
    for k in range(2):
        when(jnp.logical_and(outer, d_send[k]), c_g[k].wait_send)
        when(d_recv[k], c_i[k].wait_send)
    for k, (i, j) in enumerate(near):
        when(plain(i, j), c_p[k].wait_send)
    for c in c_wz + c_wx + c_wf[0] + c_wf[1] + c_wc:
        c.wait_send()

    @pl.when(lower)
    def _():
        for i in range(2):
            c_x[i][0].wait_send()

    @pl.when(upper)
    def _():
        for k in range(2):
            for i in range(2):
                when(d_send[k], c_x[i][1 + k].wait_send)
            when(d_send[k], c_e[k].wait_send)

    def many(count):
        return remote(ob.at[0:16 * count, :], ob.at[0:16 * count, :], A0, (w, mate))

    when(lower, many(nn - 1).wait_recv)
    when(jnp.logical_not(lower), many(nn - 2).wait_recv)
    for q, home in enumerate((upper, lower)):
        when(jnp.logical_not(home), remote(piece(of, n), px.at[q], B0 + q, (w, half - 1 + q)).wait_recv)
    out_ref[:, half * 128:(half + 1) * 128] = jnp.maximum(px[0] + px[1], 0.0).astype(BF)

    when(jnp.logical_not(lower), many(nn - 1).wait_send)
    parts = of.at[0:16 * (nn - 1), :]
    when(jnp.logical_or(upper, lower), remote(parts, parts, B0 + 2, (w, mate)).wait_send)


def solution(mesh):
    nw, nn = mesh.shape["wide"], mesh.shape["narrow"]

    def body(stored_features, channel_scale, channel_shift, first_weight, second_weight, third_weight):
        x = stored_features.reshape(512, 128)
        out = pl.pallas_call(
            functools.partial(kernel, nw, nn),
            out_shape=pltpu.VMEM((16, nn * 128), BF),
            in_specs=[pl.BlockSpec(memory_space=pl.ANY)] * 6,
            out_specs=pl.BlockSpec(memory_space=pltpu.VMEM),
            scratch_shapes=[
                pltpu.VMEM((512, 128), BF),
                pltpu.VMEM((1, 64), F32),
                pltpu.VMEM((1, 64), F32),
                pltpu.VMEM((64, 1728), BF),
                pltpu.VMEM((1728, 128), BF),
                pltpu.VMEM((512, 128), F32),
                pltpu.VMEM((6, 64, 1280), BF),
                pltpu.VMEM((6 * 192, 1280), BF),
                pltpu.VMEM((4 * 192, 1024), BF),
                pltpu.VMEM((192, 576), BF),
                pltpu.VMEM((384, 576), BF),
                pltpu.VMEM((3, 4, 64, 128), BF),
                pltpu.VMEM((3456, 256), BF),
                pltpu.VMEM((nn * 16, 3456), BF),
                pltpu.VMEM((256, 128), BF),
                pltpu.VMEM((128, 128), BF),
                pltpu.VMEM((256, 128), F32),
                pltpu.VMEM((2, 16, 128), F32),
                pltpu.SemaphoreType.DMA((NSEM,)),
                pltpu.SemaphoreType.DMA((NSEM,)),
                pltpu.SemaphoreType.REGULAR((2,)),
            ],
            compiler_params=pltpu.CompilerParams(collective_id=0, has_side_effects=True),
        )(x, channel_scale.reshape(1, 64), channel_shift.reshape(1, 64), first_weight, second_weight.T, third_weight)
        return out.reshape(16, 1, nn * 128)

    in_specs = (P(None, "wide", "narrow", None), P(), P(), P(), P(), P("narrow", None))
    return jax.shard_map(
        body, mesh=mesh, in_specs=in_specs, out_specs=P("narrow", "wide", None), check_vma=False
    )
```

```python
import functools

import jax
import jax.numpy as jnp
from jax import lax
from jax.experimental import pallas as pl
from jax.experimental.pallas import tpu as pltpu
from jax.sharding import PartitionSpec as P

BF = jnp.bfloat16
F32 = jnp.float32
MESH = pl.DeviceIdType.MESH

names = dict(H=2, D=2, G=4, P=8, WX=3, WZ=2, WF=6, WC=8, A=1, X=6, E=2, B=3, L=6)
BASE, NSEM = {}, 0
for name, size in names.items():
    BASE[name] = NSEM
    NSEM += size
H0, D0, G0, P0, WX0, WZ0, WF0, WC0, A0, X0, E0, B0, L0 = BASE.values()


def kernel(nw, nn, x_hbm, sc_hbm, sh_hbm, w1_hbm, w2_hbm, w3_hbm, out_ref,
           x_ref, sc_ref, sh_ref, w1_ref, w2_ref, xf, fb, xs1, xs2, w1p, w2p, pb, xs3, w3g, ob, rb, of, px, ssem, rsem, fsem):
    w = lax.axis_index("wide")
    n = lax.axis_index("narrow")
    half = nn // 2
    zh = n // half
    within = n % half
    mate = n + 1 - 2 * (n % 2)
    zmate = (n + half) % nn

    def xmate(k):
        return zh * half + (within + 2 * k) % half

    def side(i):
        return i - 1

    wok = [w > 0, None, w < nw - 1]
    nok = [n > 0, None, n < nn - 1]

    def ok(i, j):
        if i == 1:
            return nok[j]
        if j == 1:
            return wok[i]
        return jnp.logical_and(wok[i], nok[j])

    near = [(i, j) for i in range(3) for j in range(3) if (i, j) != (1, 1)]

    mine = pl.ds(pl.multiple_of(n * 16, 16), 16)
    loads = [
        pltpu.make_async_copy(src, dst, rsem.at[L0 + k])
        for k, (src, dst) in enumerate((
            (x_hbm, x_ref), (sc_hbm, sc_ref), (sh_hbm, sh_ref),
            (w3_hbm, w3g.at[mine, :]), (w1_hbm, w1_ref), (w2_hbm, w2_ref),
        ))
    ]
    loads[0].start()

    early = zh == 0
    late = zh == 1
    flip = (nw // 8 - 1 - w // 8) * 8 + w % 8 if nw % 8 == 0 else w
    cross = [jnp.logical_and(n == half, late), None, jnp.logical_and(n == half - 1, early)]
    same = [jnp.logical_and(nok[0], jnp.logical_not(cross[0])), None, jnp.logical_and(nok[2], jnp.logical_not(cross[2]))]

    def greet(sem, *dev):
        pl.semaphore_signal(sem, inc=1, device_id=dev, device_id_type=MESH)

    barrier = pltpu.get_barrier_semaphore()
    for k in range(1, half):
        greet(barrier, w, zh * half + (within + k) % half)
    for i in (0, 2):
        @pl.when(wok[i])
        def _():
            greet(barrier, w + side(i), n)
        for j in (0, 2):
            @pl.when(jnp.logical_and(wok[i], same[j]))
            def _():
                greet(barrier, w + side(i), n + side(j))

    @pl.when(early)
    def _():
        greet(barrier, flip, zmate)
        for k in range(half):
            greet(barrier, w, half + (within + k) % half)

    def count(cond):
        return jnp.where(cond, jnp.int32(1), jnp.int32(0))

    wcount = count(wok[0]) + count(wok[2])
    expected = half - 1 + wcount * (1 + count(same[0]) + count(same[2]))
    expected = expected + count(late) * (half + 1)

    for c in loads[1:]:
        c.start()

    @pl.when(jnp.logical_or(n == 0, n == half))
    def _():
        fb[:, :, 0:256] = jnp.zeros((6, 64, 256), BF)
        pb[:, 0] = jnp.zeros((3, 64, 128), BF)

    @pl.when(n == nn - 1)
    def _():
        fb[:, :, 768:1024] = jnp.zeros((6, 64, 256), BF)
        pb[:, 3] = jnp.zeros((3, 64, 128), BF)

    @pl.when(w == 0)
    def _():
        fb[0:2] = jnp.zeros((2, 64, 1280), BF)
        pb[0] = jnp.zeros((4, 64, 128), BF)

    @pl.when(w == nw - 1)
    def _():
        fb[4:6] = jnp.zeros((2, 64, 1280), BF)
        pb[2] = jnp.zeros((4, 64, 128), BF)

    lane = lax.broadcasted_iota(jnp.int32, (1, 128), 1)

    def shifted(t, period):
        pos = lane % period
        before = jnp.where(pos > 0, pltpu.roll(t, 1, 1), 0.0)
        after = jnp.where(pos < period - 1, pltpu.roll(t, 127, 1), 0.0)
        return before.astype(BF), t.astype(BF), after.astype(BF)

    def stack1(d, h):
        t = fb[d, :, h * 128:(h + 1) * 128].astype(F32)
        for e, v in enumerate(shifted(t, 128)):
            xs1[d * 192 + e * 64:d * 192 + (e + 1) * 64, h * 128:(h + 1) * 128] = v

    eye = lax.broadcasted_iota(jnp.int32, (64, 64), 0) == lax.broadcasted_iota(jnp.int32, (64, 64), 1)

    def column(ref):
        return jnp.sum(jnp.where(eye, ref[...], 0.0), axis=1, keepdims=True)

    for c in loads[:3]:
        c.wait()
    scale = column(sc_ref)
    shift = column(sh_ref)
    xf[...] = x_ref[...].astype(F32)
    for d in range(2):
        for h in range(4):
            t = xf[pl.ds(d * 4 + h, 64, stride=8), :]
            fb[2 + d, :, (2 + h) * 128:(3 + h) * 128] = (t * scale + shift).astype(BF)

    loads[3].wait()
    pl.semaphore_wait(barrier, expected)

    @pl.when(late)
    def _():
        greet(fsem.at[0], flip, zmate)
        for k in range(half):
            greet(fsem.at[1], w, (within + k) % half)

    def remote(src, dst, s, dev, r=None):
        return pltpu.make_async_remote_copy(
            src_ref=src, dst_ref=dst, send_sem=ssem.at[s], recv_sem=rsem.at[s if r is None else r],
            device_id=dev, device_id_type=MESH,
        )

    lo, hi = slice(256, 512), slice(512, 768)
    c_h = [
        remote(fb.at[2:4, :, lo], fb.at[2:4, :, 768:1024], H0, (w, n - 1)),
        remote(fb.at[2:4, :, hi], fb.at[2:4, :, 0:256], H0 + 1, (w, n + 1)),
    ]
    own = slice(256, 768)
    c_d = [
        remote(fb.at[2:4, :, own], fb.at[4:6, :, own], D0, (w - 1, n)),
        remote(fb.at[2:4, :, own], fb.at[0:2, :, own], D0 + 1, (w + 1, n)),
    ]
    d_send = [wok[0], wok[2]]
    d_recv = [wok[2], wok[0]]
    even = n % 2 == 0
    outer = jnp.logical_or(jnp.logical_and(even, same[0]), jnp.logical_and(jnp.logical_not(even), same[2]))

    def rows_at(on_even, on_odd):
        return pl.ds(pl.multiple_of(jnp.where(even, on_even, on_odd), 256), 256)

    outside = rows_at(0, 768)
    c_g = [
        remote(fb.at[2:4, :, outside], fb.at[4:6, :, outside], G0, (w - 1, n)),
        remote(fb.at[2:4, :, outside], fb.at[0:2, :, outside], G0 + 1, (w + 1, n)),
    ]
    depths = (slice(4, 6), slice(0, 2))
    c_i = [
        remote(fb.at[depths[k], :, rows_at(512, 256)], fb.at[depths[k], :, rows_at(0, 768)], G0 + 2 + k, (w, mate))
        for k in range(2)
    ]
    far = slice(768, 1280)
    c_x = [
        [
            remote(fb.at[2 + i:3 + i, :, own], fb.at[2 + i:3 + i, :, far], X0 + i, (w, n - 1)),
            remote(fb.at[2 + i:3 + i, :, far], fb.at[4 + i:5 + i, :, far], X0 + 2 + i, (w - 1, n)),
            remote(fb.at[2 + i:3 + i, :, far], fb.at[i:1 + i, :, far], X0 + 4 + i, (w + 1, n)),
        ]
        for i in range(2)
    ]

    def when(cond, f):
        pl.when(cond)(f)

    upper = cross[2]
    lower = cross[0]
    for i in range(2):
        when(lower, c_x[i][0].start)
    when(same[0], c_h[0].start)
    when(same[2], c_h[1].start)
    near_cut = n == half + 1
    held = [jnp.logical_and(near_cut, w == nw // 4), jnp.logical_and(near_cut, w == 3 * nw // 4 - 1)]
    for k in range(2):
        when(jnp.logical_and(d_send[k], jnp.logical_not(held[k])), c_d[k].start)

    def shard(m):
        return w3g.at[pl.ds(pl.multiple_of(m * 16, 16), 16), :]

    c_wx = [remote(shard(n), shard(n), WX0 + k - 1, (w, xmate(k))) for k in range(1, 4)]

    def half_shard(m, q):
        return w3g.at[pl.ds(pl.multiple_of(m * 16, 16), 16), (slice(0, 1792), slice(1792, 3456))[q]]

    c_wz = [remote(half_shard(n, q), half_shard(n, q), WZ0 + q, (flip, zmate)) for q in range(2)]
    c_wf = [
        [
            remote(half_shard(zmate, q), half_shard(zmate, q), WF0 + 3 * q + k - 1, (w, xmate(k)))
            for k in range(1, 4)
        ]
        for q in range(2)
    ]
    order = [n, xmate(1), xmate(2), xmate(3)]
    order = order + [(m + half) % nn for m in order]
    c_wc = [remote(shard(m), shard(m), WC0 + k, (w, mate)) for k, m in enumerate(order)]
    for q in range(2):
        when(late, c_wz[q].start)
    for c in c_wx:
        c.start()
    c_wc[0].start()

    loads[4].wait()
    loads[5].wait()
    for a in range(3):
        for b in range(3):
            c0 = (a * 3 + b) * 192
            w1p[b * 64:(b + 1) * 64, a * 192:(a + 1) * 192] = w1_ref[:, c0:c0 + 192]
            w2p[b * 128:(b + 1) * 128, a * 192:(a + 1) * 192] = w2_ref[c0:c0 + 192, :].T
    for d in (2, 3):
        for h in range(2, 6):
            stack1(d, h)

    def edge_rows(depths, j):
        for d in depths:
            for h in ((0, 1), (6, 7))[j]:
                stack1(d, h)

    for j in range(2):
        when(same[2 * j], c_h[1 - j].wait_recv)
    for k in range(2):
        when(jnp.logical_and(d_send[k], held[k]), c_d[k].start)
    for k in range(2):
        when(jnp.logical_and(outer, d_send[k]), c_g[k].start)
    @pl.when(early)
    def _():
        pl.semaphore_wait(fsem.at[0], 1)
        for c in c_wz:
            c.start()

    edge_rows((2, 3), 0)
    when(jnp.logical_not(upper), lambda: edge_rows((2, 3), 1))
    for k in range(2):
        @pl.when(d_recv[k])
        def _():
            c_d[k].wait_recv()
            c_i[k].start()
    for d in (0, 1, 4, 5):
        for h in range(2, 6):
            stack1(d, h)
    for k in range(2):
        when(d_recv[k], c_i[k].wait_recv)
        when(jnp.logical_and(outer, d_recv[k]), c_g[k].wait_recv)
    edge_rows((0, 1, 4, 5), 0)
    when(jnp.logical_not(upper), lambda: edge_rows((0, 1, 4, 5), 1))

    def spread():
        for q in range(2):
            c_wz[q].wait_recv()
            for c in c_wf[q]:
                c.start()
        for k in range(3):
            c_wx[k].wait_recv()
        for k in range(1, 5):
            c_wc[k].start()

    def first(h0, rows):
        row = h0 * 128 + lax.broadcasted_iota(jnp.int32, (1, rows * 128), 1)
        inside = jnp.logical_and(
            jnp.logical_or(row >= 128, n > 0), jnp.logical_or(row < 640, n < nn - 1)
        )
        span = rows * 128

        def level(d, carry):
            y = jnp.dot(
                w1p[...],
                xs1[pl.ds(pl.multiple_of(d * 192, 192), 576), h0 * 128:h0 * 128 + span + 256],
                preferred_element_type=F32,
            )
            y = y[0:64, 0:span] + y[64:128, 128:span + 128] + y[128:192, 256:span + 256]
            depth = 2 * w + d - 1
            keep = jnp.logical_and(inside, jnp.logical_and(depth >= 0, depth < 2 * nw))
            y = jnp.where(keep, jnp.maximum(y, 0.0), 0.0)
            for h in range(rows):
                for e, v in enumerate(shifted(y[:, h * 128:(h + 1) * 128], 128)):
                    c0 = (h0 + h) * 128
                    xs2[pl.ds(pl.multiple_of(d * 192 + e * 64, 64), 64), c0:c0 + 128] = v
            return carry

        lax.fori_loop(0, 4, level, 0)

    def second(h0, rows):
        span = rows * 128

        def level(d):
            y = jnp.dot(
                w2p[...], xs2[d * 192:d * 192 + 576, h0 * 128:h0 * 128 + span + 256],
                preferred_element_type=F32,
            )
            return y[0:128, 0:span] + y[128:256, 128:span + 128] + y[256:384, 256:span + 256]

        s = jnp.maximum(jnp.maximum(level(0), level(1)), 0.0)
        out = []
        for r in range(rows // 2):
            t = jnp.maximum(s[:, r * 256:r * 256 + 128], s[:, r * 256 + 128:r * 256 + 256])
            out.append(jnp.maximum(t, pltpu.roll(t, 127, 1)).astype(BF))
        return out

    k_i = lax.broadcasted_iota(jnp.int32, (128, 128), 0)
    j_i = lax.broadcasted_iota(jnp.int32, (128, 128), 1)

    picks = [jnp.where(k_i == 2 * (j_i - 64 * q), 1.0, 0.0).astype(BF) for q in range(2)]

    def pack(t):
        return jnp.dot(t[0:64], picks[0], preferred_element_type=F32) + jnp.dot(
            t[64:128], picks[1], preferred_element_type=F32
        )

    @pl.when(jnp.logical_not(upper))
    def _():
        when(late, spread)
        first(0, 6)
        r0, r1 = second(0, 4)
        keep = jnp.where(lower, 0.0, 1.0)
        pb[1, 1] = (pack(r0) * keep).astype(BF)
        pb[1, 2] = pack(r1).astype(BF)

    @pl.when(upper)
    def _():
        for a in range(3):
            xs3[a * 1152 + 768:(a + 1) * 1152, 128:256] = jnp.zeros((384, 128), BF)
        first(0, 4)
        for i in range(2):
            c_x[i][0].wait_recv()
            for k in range(2):
                when(d_send[k], c_x[i][1 + k].start)
        for d in (2, 3):
            for h in range(6, 10):
                stack1(d, h)
        rb[...] = second(0, 2)[0]
        spread()
        for k in range(2):
            for i in range(2):
                when(d_recv[k], c_x[i][1 + k].wait_recv)
        for d in (0, 1, 4, 5):
            for h in range(6, 10):
                stack1(d, h)
        first(4, 4)
        r1, r2 = second(2, 4)
        pb[1, 1] = pack(rb[...]).astype(BF)
        pb[1, 2] = pack(r1).astype(BF)
        pb[1, 3] = pack(r2).astype(BF)

    def beside(i, j):
        if j == 1:
            return wok[i]
        if i == 1:
            return same[j]
        return jnp.logical_and(wok[i], same[j])

    c_e = [
        remote(pb.at[1, 1:4], pb.at[2, 1:4], E0, (w - 1, n)),
        remote(pb.at[1, 1:4], pb.at[0, 1:4], E0 + 1, (w + 1, n)),
    ]
    c_p = []
    for k, (i, j) in enumerate(near):
        src, dst = ((slice(1, 2), slice(3, 4)), (slice(1, 3), slice(1, 3)), (slice(2, 3), slice(0, 1)))[j]
        c_p.append(
            remote(pb.at[1, src], pb.at[2 - i, dst], P0 + k, (w + side(i), n + side(j)))
        )

    def plain(i, j):
        return jnp.logical_and(beside(i, j), jnp.logical_not(upper)) if j == 1 else beside(i, j)

    for k in range(2):
        when(jnp.logical_and(upper, d_send[k]), c_e[k].start)
    for k, (i, j) in enumerate(near):
        when(plain(i, j), c_p[k].start)

    def spread_rest():
        for k in range(3):
            for q in range(2):
                c_wf[q][k].wait_recv()
            c_wc[7 - k].start()

    when(jnp.logical_and(early, jnp.logical_not(upper)), spread)
    when(late, spread_rest)
    for k, (i, j) in enumerate(near):
        when(plain(2 - i, 2 - j), c_p[k].wait_recv)

    low = lane < 64

    @pl.when(upper)
    def _():
        for k in range(2):
            when(d_recv[k], c_e[k].wait_recv)

    def coarse_stack(first_row, taps, dst, cols):
        def level(a, carry):
            q = [pb[a, first_row + r].astype(F32) if first_row + r < 4 else jnp.zeros((64, 128), F32) for r in range(taps + 1)]
            z = [pltpu.roll(v, 64, 1) for v in q]
            for b in range(taps):
                for c in range(2):
                    t = jnp.where(low, q[b], z[b + 1]) if c == 0 else jnp.where(low, z[b], q[b + 1])
                    for e, v in enumerate(shifted(t, 64)):
                        r0 = (b * 3 + e) * 128 + c * 64
                        dst[pl.ds(pl.multiple_of(a * 1152 + r0, 64), 64), cols] = v
            return carry

        lax.fori_loop(0, 3, level, 0)

    coarse_stack(0, 3, xs3, slice(0, 128))
    when(upper, lambda: coarse_stack(2, 2, xs3, slice(128, 256)))

    for c in c_wc[:4]:
        c.wait_recv()

    @pl.when(late)
    def _():
        for c in c_wc[4:]:
            c.wait_recv()

    def coarse(g):
        rows = slice(g * 128, (g + 1) * 128)

        @pl.when(jnp.logical_not(upper))
        def _():
            y = jnp.dot(w3g[rows, :], xs3[:, 0:128], preferred_element_type=F32)

            @pl.when(lower)
            def _():
                of[rows, :] = y

            @pl.when(jnp.logical_not(lower))
            def _():
                ob[rows, :] = jnp.maximum(y, 0.0).astype(BF)

        @pl.when(upper)
        def _():
            y = jnp.dot(w3g[rows, :], xs3[...], preferred_element_type=F32)
            ob[rows, :] = jnp.maximum(y[:, 0:128], 0.0).astype(BF)
            of[rows, :] = y[:, 128:256]

    def block(m):
        return out_ref.at[:, pl.ds(pl.multiple_of(m * 128, 128), 128)]

    def piece(ref, m):
        return ref.at[pl.ds(pl.multiple_of(m * 16, 16), 16), :]

    def sends(m):
        return (
            remote(piece(ob, m), block(n), A0, (w, m)),
            remote(piece(of, m), px.at[0], B0 + 2, (w, m), r=B0),
            remote(piece(of, m), px.at[1], B0 + 2, (w, m), r=B0 + 1),
        )

    for g in range(2):
        if g == 1:
            @pl.when(early)
            def _():
                spread_rest()
                for c in c_wc[4:]:
                    c.wait_recv()
                pl.semaphore_wait(fsem.at[1], half)
        coarse(g)
        group = range(g * half, (g + 1) * half)

        @pl.when(jnp.logical_not(lower))
        def _():
            for m in group:
                when(m != n, sends(m)[0].start)

        for q, home in enumerate((upper, lower)):
            @pl.when(home)
            def _():
                for m in group:
                    if m != half - 1 + q:
                        sends(m)[1 + q].start()

    @pl.when(jnp.logical_not(lower))
    def _():
        out_ref[:, pl.ds(pl.multiple_of(n * 128, 128), 128)] = ob[mine, :]

    @pl.when(upper)
    def _():
        px[0] = of[mine, :]

    @pl.when(lower)
    def _():
        px[1] = of[mine, :]

    when(same[0], c_h[0].wait_send)
    when(same[2], c_h[1].wait_send)
    for k in range(2):
        when(d_send[k], c_d[k].wait_send)
    for k in range(2):
        when(jnp.logical_and(outer, d_send[k]), c_g[k].wait_send)
        when(d_recv[k], c_i[k].wait_send)
    for k, (i, j) in enumerate(near):
        when(plain(i, j), c_p[k].wait_send)
    for c in c_wz + c_wx + c_wf[0] + c_wf[1] + c_wc:
        c.wait_send()

    @pl.when(lower)
    def _():
        for i in range(2):
            c_x[i][0].wait_send()

    @pl.when(upper)
    def _():
        for k in range(2):
            for i in range(2):
                when(d_send[k], c_x[i][1 + k].wait_send)
            when(d_send[k], c_e[k].wait_send)

    def many(count):
        return remote(ob.at[0:16 * count, :], ob.at[0:16 * count, :], A0, (w, mate))

    when(lower, many(nn - 1).wait_recv)
    when(jnp.logical_not(lower), many(nn - 2).wait_recv)
    for q, home in enumerate((upper, lower)):
        when(jnp.logical_not(home), remote(piece(of, n), px.at[q], B0 + q, (w, half - 1 + q)).wait_recv)
    out_ref[:, half * 128:(half + 1) * 128] = jnp.maximum(px[0] + px[1], 0.0).astype(BF)

    when(jnp.logical_not(lower), many(nn - 1).wait_send)
    parts = of.at[0:16 * (nn - 1), :]
    when(jnp.logical_or(upper, lower), remote(parts, parts, B0 + 2, (w, mate)).wait_send)


def solution(mesh):
    nw, nn = mesh.shape["wide"], mesh.shape["narrow"]

    def body(stored_features, channel_scale, channel_shift, first_weight, second_weight, third_weight):
        x = stored_features.reshape(512, 128)
        out = pl.pallas_call(
            functools.partial(kernel, nw, nn),
            out_shape=pltpu.VMEM((16, nn * 128), BF),
            in_specs=[pl.BlockSpec(memory_space=pl.ANY)] * 6,
            out_specs=pl.BlockSpec(memory_space=pltpu.VMEM),
            scratch_shapes=[
                pltpu.VMEM((512, 128), BF),
                pltpu.VMEM((1, 64), F32),
                pltpu.VMEM((1, 64), F32),
                pltpu.VMEM((64, 1728), BF),
                pltpu.VMEM((1728, 128), BF),
                pltpu.VMEM((512, 128), F32),
                pltpu.VMEM((6, 64, 1280), BF),
                pltpu.VMEM((6 * 192, 1280), BF),
                pltpu.VMEM((4 * 192, 1024), BF),
                pltpu.VMEM((192, 576), BF),
                pltpu.VMEM((384, 576), BF),
                pltpu.VMEM((3, 4, 64, 128), BF),
                pltpu.VMEM((3456, 256), BF),
                pltpu.VMEM((nn * 16, 3456), BF),
                pltpu.VMEM((256, 128), BF),
                pltpu.VMEM((128, 128), BF),
                pltpu.VMEM((256, 128), F32),
                pltpu.VMEM((2, 16, 128), F32),
                pltpu.SemaphoreType.DMA((NSEM,)),
                pltpu.SemaphoreType.DMA((NSEM,)),
                pltpu.SemaphoreType.REGULAR((2,)),
            ],
            compiler_params=pltpu.CompilerParams(collective_id=0, has_side_effects=True),
        )(x, channel_scale.reshape(1, 64), channel_shift.reshape(1, 64), first_weight, second_weight.T, third_weight)
        return out.reshape(16, 1, nn * 128)

    in_specs = (P(None, "wide", "narrow", None), P(), P(), P(), P(), P("narrow", None))
    return jax.shard_map(
        body, mesh=mesh, in_specs=in_specs, out_specs=P("narrow", "wide", None), check_vma=False
    )
```
